32 devices in a mesh: dp: 16 (over z, x, core), mp: 2 (over y).
Axes of the slice: x: 2, y: 2, z: 4, core: 2. Of those that a mesh axis runs over, the one named last changes fastest.
Arguments:
- inputs: bfloat16 [32768, 1152], P(('dp', 'mp')), may hold values from -6 to 6
- picture_start: int32 [32768], P('dp'), may hold values from 0 to 31744, as said below
- prenorm_gain: float32 [1152], replicated, may hold values from 0.5 to 1.5
- prenorm_shift: float32 [1152], replicated, may hold values from -2 to 2
- query_weight: bfloat16 [1152, 1152], P('dp', 'mp'), may hold values from -1 to 1
- query_bias: float32 [1152], P('mp'), may hold values from -2 to 2
- key_weight: bfloat16 [1152, 1152], P('dp', 'mp'), may hold values from -0.1875 to 0.1875
- value_weight: bfloat16 [1152, 1152], P('dp', 'mp'), may hold values from -0.1875 to 0.1875
- value_bias: float32 [1152], P('mp'), may hold values from -2 to 2
- output_weight: bfloat16 [1152, 1152], P('mp', 'dp'), may hold values from -0.75 to 0.75
- output_bias: float32 [1152], replicated, may hold values from -2 to 2
- midnorm_gain: float32 [1152], replicated, may hold values from 0.5 to 1.5
- midnorm_shift: float32 [1152], replicated, may hold values from -2 to 2
- hidden_weight: bfloat16 [1152, 4304], P('dp', 'mp'), may hold values from -0.1875 to 0.1875
- hidden_bias: float32 [4304], P('mp'), may hold values from -2 to 2
- project_weight: bfloat16 [4304, 1152], P('mp', 'dp'), may hold values from -0.09375 to 0.09375
- project_bias: float32 [1152], replicated, may hold values from -2 to 2
- cotangent: bfloat16 [32768, 1152], P(('dp', 'mp')), may hold values from -6 to 6
Outputs:
- layer_output: bfloat16 [32768, 1152], P(('dp', 'mp'))
- inputs_gradient: float32 [32768, 1152], P(('dp', 'mp'))
- prenorm_gain_gradient: float32 [1152], replicated
- prenorm_shift_gradient: float32 [1152], replicated
- query_weight_gradient: float32 [1152, 1152], P('dp', 'mp')
- query_bias_gradient: float32 [1152], P('mp')
- key_weight_gradient: float32 [1152, 1152], P('dp', 'mp')
- value_weight_gradient: float32 [1152, 1152], P('dp', 'mp')
- value_bias_gradient: float32 [1152], P('mp')
- output_weight_gradient: float32 [1152, 1152], P('mp', 'dp')
- output_bias_gradient: float32 [1152], replicated
- midnorm_gain_gradient: float32 [1152], replicated
- midnorm_shift_gradient: float32 [1152], replicated
- hidden_weight_gradient: float32 [1152, 4304], P('dp', 'mp')
- hidden_bias_gradient: float32 [4304], P('mp')
- project_weight_gradient: float32 [4304, 1152], P('mp', 'dp')
- project_bias_gradient: float32 [1152], replicated
- logit_peak: float32 [16], P('mp')
- clipped_query: float32 [1152, 1152], P('dp', 'mp')
- clipped_key: float32 [1152, 1152], P('dp', 'mp')
The draws below stay inside these ranges and needn't reach their ends.
Inputs may be any that keep to these rules, and one draw needn't show every extreme that they name: `picture_start`: for each patch, the index in the whole array of the first patch of its picture. A picture is a run of consecutive patches inside one packed row of 2048 patches (rows begin at multiples of 2048); each picture has 100 to 1024 patches, and every row ends with one picture of exactly 1024 patches.
All inputs are finite; a program needn't handle non-finite values.
Results may differ from the reference program's by a relative error of at most 0.018.
Values may be sent and summed in bfloat16 or wider, within the bound.
A program may use at most 256 MiB of HBM per device.

```python
import math
import jax
import jax.numpy as jnp
from jax import lax

D = 1152
HEADS = 16
HEAD = 72
FF = 4304
ROW = 2048
PIC_MIN = 100
PIC_MAX = 1024
TOKENS = 32768


def picture_row(row_key):
    count_key = jax.random.fold_in(row_key, 11)
    share_key = jax.random.fold_in(row_key, 12)
    order_key = jax.random.fold_in(row_key, 13)
    most_pictures = min(10, PIC_MAX // PIC_MIN)
    picture_count = jax.random.randint(count_key, (), 1, most_pictures + 1)
    slot_index = jnp.arange(11, dtype=jnp.int32)
    shares = jnp.where(slot_index < picture_count, jax.random.randint(share_key, (11,), 1, 1000), 0)
    spare = PIC_MAX - PIC_MIN * picture_count
    extras = spare * shares // jnp.sum(shares)
    extras = extras + jnp.where(slot_index == picture_count - 1, spare - jnp.sum(extras), 0)
    picture_sizes = jnp.where(slot_index < picture_count, PIC_MIN + extras, 0).astype(jnp.int32)
    picture_sizes = picture_sizes[jax.random.permutation(order_key, 11)]
    picture_sizes = jnp.concatenate([picture_sizes, jnp.full((1,), PIC_MAX, jnp.int32)])
    picture_ends = jnp.cumsum(picture_sizes)
    picture_begins = picture_ends - picture_sizes
    places = jnp.arange(ROW, dtype=jnp.int32)
    inside = (places[:, None] >= picture_begins[None, :]) & (places[:, None] < picture_ends[None, :])
    return jnp.sum(jnp.where(inside, picture_begins[None, :], 0), axis=1).astype(jnp.int32)


def draw_picture_start(key, part):
    row_count = TOKENS // ROW
    local_starts = jax.vmap(picture_row)(jax.random.split(key, row_count))
    offsets = jnp.arange(row_count, dtype=jnp.int32)[:, None] * ROW
    return (local_starts + offsets).reshape(TOKENS).astype(jnp.int32)


def draw_query_weight(key, part):
    entries = jax.random.truncated_normal(jax.random.fold_in(key, 21), -3.0, 3.0, (D, D), jnp.float32)
    head_scale = jnp.exp(jax.random.uniform(jax.random.fold_in(key, 22), (HEADS,), jnp.float32, math.log(0.5), math.log(2.5)))
    column_scale = jnp.repeat(head_scale, HEAD)
    return (entries * (1.0 / math.sqrt(D)) * column_scale[None, :]).astype(jnp.bfloat16)


def steps_of(rng, extent, shards, smallest, top_value):
    def one(axis_at, blocks):
        steps = jax.random.uniform(jax.random.fold_in(jax.random.fold_in(rng, 6), axis_at), (blocks,), jnp.float32, smallest / len(shards), top_value / len(shards))
        return jnp.repeat(jnp.exp(steps), extent[axis_at] // blocks).reshape((-1,) + (1,) * (len(extent) - axis_at - 1))

    loudness = one(*shards[0])
    for cut in shards[1:]:
        loudness = loudness * one(*cut)
    return loudness


def gaussian(stream_key, shape, width, most, cuts=(), held_as=jnp.bfloat16):
    drawn = width * jax.random.normal(stream_key, shape, jnp.float32)
    if cuts:
        drawn = drawn * steps_of(stream_key, shape, cuts, -0.22, 0.18)
    return jnp.clip(drawn, -most, most).astype(held_as)


def setup_inputs(seed: int = 0) -> dict:
    splits = jax.random.split(jax.random.key(seed), 19)
    inputs = gaussian(splits[0], (TOKENS, D), 1.0, 6.0, ((0, 32),))
    picture_start = draw_picture_start(jax.random.fold_in(splits[18], 71), 0)
    prenorm_gain = jnp.clip(1.0 + 0.1 * jax.random.normal(splits[2], (D,), jnp.float32), 0.5, 1.5)
    prenorm_shift = gaussian(splits[3], (D,), 0.3, 2.0, (), jnp.float32)
    query_weight = draw_query_weight(jax.random.fold_in(splits[18], 71), 0)
    query_bias = gaussian(splits[5], (D,), 0.3, 2.0, ((0, 2),), jnp.float32)
    key_weight = gaussian(splits[6], (D, D), D ** -0.5, 0.1875, ((0, 16), (1, 2)))
    value_weight = gaussian(splits[7], (D, D), D ** -0.5, 0.1875, ((0, 16), (1, 2)))
    value_bias = gaussian(splits[8], (D,), 0.3, 2.0, ((0, 2),), jnp.float32)
    output_weight = gaussian(splits[9], (D, D), (D // 16) ** -0.5, 0.75, ((0, 2), (1, 16)))
    output_bias = gaussian(splits[10], (D,), 0.3, 2.0, (), jnp.float32)
    midnorm_gain = jnp.clip(1.0 + 0.1 * jax.random.normal(splits[11], (D,), jnp.float32), 0.5, 1.5)
    midnorm_shift = gaussian(splits[12], (D,), 0.3, 2.0, (), jnp.float32)
    hidden_weight = gaussian(splits[13], (D, FF), D ** -0.5, 0.1875, ((0, 16), (1, 2)))
    hidden_bias = gaussian(splits[14], (FF,), 0.3, 2.0, ((0, 2),), jnp.float32)
    project_weight = gaussian(splits[15], (FF, D), FF ** -0.5, 0.09375, ((0, 2), (1, 16)))
    project_bias = gaussian(splits[16], (D,), 0.3, 2.0, (), jnp.float32)
    cotangent = gaussian(splits[17], (TOKENS, D), 1.0, 6.0, ((0, 32),))
    return dict(inputs=inputs, picture_start=picture_start, prenorm_gain=prenorm_gain, prenorm_shift=prenorm_shift, query_weight=query_weight, query_bias=query_bias, key_weight=key_weight, value_weight=value_weight, value_bias=value_bias, output_weight=output_weight, output_bias=output_bias, midnorm_gain=midnorm_gain, midnorm_shift=midnorm_shift, hidden_weight=hidden_weight, hidden_bias=hidden_bias, project_weight=project_weight, project_bias=project_bias, cotangent=cotangent)


EPSILON = 1e-06
CLIP_LIMIT = 7.0
MASKED_SCORE = -1e+30

@jax.custom_vjp
def low(v):
    return lax.optimization_barrier(v.astype(jnp.bfloat16)).astype(jnp.float32)

@jax.custom_vjp
def low_back(v):
    return v

def low_keep(v):
    return (low(v), None)

def low_pass(kept, grad):
    return (grad,)

def back_keep(v):
    return (v, None)

def back_low(kept, grad):
    return (low(grad),)
low.defvjp(low_keep, low_pass)
low_back.defvjp(back_keep, back_low)

def matmul(left, right):
    return jnp.dot(left, right, precision=lax.Precision.HIGHEST, preferred_element_type=jnp.float32)

def layer_norm(values, gain, shift):
    centre = lax.optimization_barrier(jnp.mean(values, axis=-1, keepdims=True))
    centred = values - centre
    spread = lax.optimization_barrier(jnp.mean(centred * centred, axis=-1, keepdims=True))
    return centred * lax.rsqrt(spread + EPSILON) * gain + shift

def attend(queries, keys, values, starts):
    length = queries.shape[0]
    query_heads = queries.reshape(length, HEADS, HEAD)
    key_heads = keys.reshape(length, HEADS, HEAD)
    value_heads = values.reshape(length, HEADS, HEAD)
    raw_scores = jnp.einsum('qhd,khd->hqk', query_heads, key_heads, precision=lax.Precision.HIGHEST) * HEAD ** (-0.5)
    scores = low_back(raw_scores)
    allowed = starts[:, None] == starts[None, :]
    masked = jnp.where(allowed[None], scores, MASKED_SCORE)
    row_top = lax.optimization_barrier(jnp.max(masked, axis=2, keepdims=True))
    log_total = row_top + jnp.log(lax.optimization_barrier(jnp.sum(jnp.exp(masked - row_top), axis=2, keepdims=True)))
    weights = low(jnp.exp(masked - log_total))
    mixed = jnp.einsum('hqk,khd->qhd', weights, value_heads, precision=lax.Precision.HIGHEST)
    return (mixed.reshape(length, D), lax.optimization_barrier(jnp.max(row_top, axis=(1, 2))))

def layer_row(params, row_inputs, row_starts):
    prenorm_gain, prenorm_shift, query_weight, query_bias, key_weight, value_weight, value_bias, output_weight, output_bias, midnorm_gain, midnorm_shift, hidden_weight, hidden_bias, project_weight, project_bias = params
    attn_in = low(layer_norm(row_inputs, prenorm_gain, prenorm_shift))
    queries = low_back(low(matmul(attn_in, query_weight) + query_bias))
    keys = low_back(low(matmul(attn_in, key_weight)))
    values = low_back(low(matmul(attn_in, value_weight) + value_bias))
    mixed, peaks = attend(queries, keys, values, row_starts)
    mixed = low_back(low(mixed))
    residual_mid = row_inputs + low_back(matmul(mixed, output_weight) + output_bias)
    mlp_in = low(layer_norm(residual_mid, midnorm_gain, midnorm_shift))
    up_rows = low_back(matmul(mlp_in, hidden_weight) + hidden_bias)
    activated = low(jax.nn.gelu(up_rows, approximate=True))
    return (residual_mid + matmul(activated, project_weight) + project_bias, peaks)

def run_rows(rows_in, params, starts):

    def one_row(carried, item):
        out_row, peaks = jax.checkpoint(layer_row)(params, item[0], item[1])
        return (carried, (out_row, peaks))
    unused, (outs, peaks) = lax.scan(one_row, jnp.zeros((), jnp.float32), (rows_in, starts))
    return (outs, lax.optimization_barrier(jnp.max(peaks, axis=0)))

def reference(inputs, picture_start, prenorm_gain, prenorm_shift, query_weight, query_bias, key_weight, value_weight, value_bias, output_weight, output_bias, midnorm_gain, midnorm_shift, hidden_weight, hidden_bias, project_weight, project_bias, cotangent):
    row_count = TOKENS // ROW
    params = tuple((item.astype(jnp.float32) for item in (prenorm_gain, prenorm_shift, query_weight, query_bias, key_weight, value_weight, value_bias, output_weight, output_bias, midnorm_gain, midnorm_shift, hidden_weight, hidden_bias, project_weight, project_bias)))
    rows_in = inputs.astype(jnp.float32).reshape(row_count, ROW, D)
    starts = picture_start.astype(jnp.int32).reshape(row_count, ROW)

    def forward(rows_value, params_value):
        return run_rows(rows_value, params_value, starts)
    outs, pullback, peak = jax.vjp(forward, rows_in, params, has_aux=True)
    grad_rows, grads = pullback(cotangent.astype(jnp.float32).reshape(row_count, ROW, D))
    factor = jnp.sqrt(CLIP_LIMIT / jnp.maximum(peak, CLIP_LIMIT))
    columns = jnp.repeat(factor, HEAD)
    clipped_query = query_weight.astype(jnp.float32) * columns[None, :]
    clipped_key = key_weight.astype(jnp.float32) * columns[None, :]
    return (outs.reshape(TOKENS, D).astype(jnp.bfloat16), grad_rows.reshape(TOKENS, D), grads[0], grads[1], grads[2], grads[3], grads[4], grads[5], grads[6], grads[7], grads[8], grads[9], grads[10], grads[11], grads[12], grads[13], grads[14], peak, clipped_query, clipped_key)
```

```python
import math
from functools import partial

import jax
import jax.numpy as jnp
from jax import lax
from jax.experimental import pallas as pl
from jax.experimental.pallas import tpu as pltpu
from jax.sharding import PartitionSpec as P

HEAD = 72
HEADS = 16
ROW = 2048
HALF = 1024
EPSILON = 1e-06
CLIP_LIMIT = 7.0
MASKED_SCORE = -1e30
FEATURES = 16
PICTURES = 10
QUERY_BLOCK = 256
SCALE = HEAD ** (-0.5)
LOG2E = 1.0 / math.log(2.0)
EXPONENT = SCALE * LOG2E
F32 = jnp.float32
BF16 = jnp.bfloat16


def dot(left, right, left_dim=1, right_dim=0):
    return lax.dot_general(
        left, right, (((left_dim,), (right_dim,)), ((), ())), preferred_element_type=F32
    )


def split_terms(value, count):
    terms = []
    for _ in range(count):
        term = value.astype(BF16).astype(F32)
        terms.append(term)
        value = value - term
    return terms


def query_operand(query, features):
    pad = jnp.zeros((8, query.shape[1]), F32)
    high, low = split_terms(query.astype(F32) * EXPONENT, 2)
    return jnp.concatenate([high, pad, low, pad, features], axis=0).astype(BF16)


def key_operand(key, features):
    pad = jnp.zeros((8, key.shape[1]), F32)
    wide = key.astype(F32)
    stacked = jnp.concatenate([wide, pad, wide, pad, features], axis=0)
    return stacked.T.astype(BF16)


def rows_below(wide, extra):
    width = wide.shape[1]
    row = lax.broadcasted_iota(jnp.int32, (8, width), 0)
    block = jnp.zeros((8, width), F32)
    for position, line in enumerate(extra):
        block = jnp.where(row == position, line, block)
    return jnp.concatenate([wide, block], axis=0)


def forward_kernel(mask_ref, key_mask_ref, query_ref, key_ref, value_ref, mixed_ref, log_ref, top_ref):
    query_rows = query_operand(query_ref[0, 0], mask_ref[...])
    key_rows = key_operand(key_ref[0, 0], key_mask_ref[...])
    value_rows = rows_below(value_ref[0, 0].astype(F32), [jnp.ones((1, 1), F32)]).astype(BF16)
    for begin in range(0, HALF, QUERY_BLOCK):
        block = slice(begin, begin + QUERY_BLOCK)
        scores = dot(key_rows, query_rows[:, block])
        top = jnp.max(scores, axis=0, keepdims=True)
        weights = jnp.exp2(scores - top).astype(BF16)
        summed = dot(value_rows, weights)
        total = summed[HEAD : HEAD + 1]
        mixed_ref[0, :, block] = (summed[:HEAD] / total).astype(BF16)
        log_ref[0, :, block] = top + jnp.log2(total)
        top_ref[0, :, block] = top


def backward_kernel(
    mask_ref, key_mask_ref, query_ref, key_ref, value_ref, mixed_ref, log_ref, grad_ref, out_ref
):
    query, key = query_ref[0, 0], key_ref[0, 0]
    grad = grad_ref[0]
    row = lax.broadcasted_iota(jnp.int32, (FEATURES, HALF), 0)
    features = mask_ref[...]
    for position, term in enumerate(split_terms(-log_ref[0], 3)):
        features = jnp.where(row == PICTURES + position, term, features)
    query_rows = query_operand(query, features)
    key_rows = key_operand(key, key_mask_ref[...])
    grad_wide = grad.astype(F32)
    delta = jnp.sum(grad_wide * mixed_ref[0].astype(F32), axis=0, keepdims=True)
    grad_rows = rows_below(grad_wide, split_terms(-delta, 2)).astype(BF16)
    one = jnp.ones((1, 1), F32)
    value_rows = rows_below(value_ref[0, 0].astype(F32), [one, one]).T.astype(BF16)
    query_cols = query.astype(F32).T.astype(BF16)
    grad_cols = grad_wide.T.astype(BF16)
    grad_key = jnp.zeros((HALF, HEAD), F32)
    grad_value = jnp.zeros((HALF, HEAD), F32)
    for begin in range(0, HALF, QUERY_BLOCK):
        block = slice(begin, begin + QUERY_BLOCK)
        weights = jnp.exp2(dot(key_rows, query_rows[:, block]))
        slopes = dot(value_rows, grad_rows[:, block])
        grad_scores = (weights * slopes).astype(BF16)
        grad_value = grad_value + dot(weights.astype(BF16), grad_cols[block])
        grad_key = grad_key + dot(grad_scores, query_cols[block])
        out_ref[0, 0, :, block] = (dot(key, grad_scores) * SCALE).astype(BF16)
    out_ref[1, 0] = (grad_key * SCALE).T.astype(BF16)
    out_ref[2, 0] = grad_value.T.astype(BF16)


def head_specs():
    features = pl.BlockSpec((FEATURES, HALF), lambda h: (0, 0))
    part = [pl.BlockSpec((1, 1, HEAD, HALF), lambda h, i=i: (i, h, 0, 0)) for i in range(3)]
    head = pl.BlockSpec((1, HEAD, HALF), lambda h: (h, 0, 0))
    line = pl.BlockSpec((1, 1, HALF), lambda h: (h, 0, 0))
    return features, part, head, line


def attention_forward(masks, stacked):
    heads = stacked.shape[1]
    features, part, head, line = head_specs()
    area = heads * HALF * HALF
    return pl.pallas_call(
        forward_kernel,
        grid=(heads,),
        in_specs=[features, features, *part],
        out_specs=(head, line, line),
        out_shape=(
            jax.ShapeDtypeStruct((heads, HEAD, HALF), BF16),
            jax.ShapeDtypeStruct((heads, 1, HALF), F32),
            jax.ShapeDtypeStruct((heads, 1, HALF), F32),
        ),
        cost_estimate=pl.CostEstimate(
            flops=area * 2 * 256 * 2, bytes_accessed=heads * HALF * HEAD * 8, transcendentals=area
        ),
        name="attention_forward",
    )(*masks, stacked, stacked, stacked)


def attention_backward(masks, stacked, mixed, logs, grads):
    heads = stacked.shape[1]
    features, part, head, line = head_specs()
    area = heads * HALF * HALF
    return pl.pallas_call(
        backward_kernel,
        grid=(heads,),
        in_specs=[features, features, *part, head, line, head],
        out_specs=pl.BlockSpec((3, 1, HEAD, HALF), lambda h: (0, h, 0, 0)),
        out_shape=jax.ShapeDtypeStruct((3, heads, HEAD, HALF), BF16),
        cost_estimate=pl.CostEstimate(
            flops=area * 2 * 256 * 5, bytes_accessed=heads * HALF * HEAD * 16, transcendentals=area
        ),
        name="attention_backward",
    )(*masks, stacked, stacked, stacked, mixed, logs, grads)


def picture_masks(starts):
    before = jnp.concatenate([starts[:1], starts[:-1]])
    changes = (starts != before).astype(F32)
    place = lax.iota(jnp.int32, HALF)
    number = jnp.sum(jnp.where(place[:, None] <= place[None, :], changes[:, None], 0.0), axis=0)
    row = lax.broadcasted_iota(jnp.int32, (FEATURES, HALF), 0)
    same = row.astype(F32) == number[None, :]
    listed = row < PICTURES
    mask = jnp.where(listed & ~same, MASKED_SCORE, 0.0)
    key_mask = jnp.where(listed, same.astype(F32), (row < PICTURES + 3).astype(F32))
    return mask, key_mask


def local_norm(values):
    centre = jnp.mean(values, axis=1, keepdims=True)
    centred = values - centre
    rstd = lax.rsqrt(jnp.mean(centred * centred, axis=1, keepdims=True) + EPSILON)
    return centred * rstd, rstd


def norm_backward(grad_normed, normed, rstd, gain):
    scaled = grad_normed * gain
    mean_grad = jnp.mean(scaled, axis=1, keepdims=True)
    mean_cross = jnp.mean(scaled * normed, axis=1, keepdims=True)
    return rstd * (scaled - mean_grad - normed * mean_cross)


def gelu_parts(rows):
    cubic = math.sqrt(2.0 / math.pi) * (rows + 0.044715 * rows * rows * rows)
    bend = jnp.tanh(cubic)
    value = 0.5 * rows * (1.0 + bend)
    slope = 0.5 * (1.0 + bend) + 0.5 * rows * (1.0 - bend * bend) * (
        math.sqrt(2.0 / math.pi) * (1.0 + 3.0 * 0.044715 * rows * rows)
    )
    return value, slope


def total(parts):
    out = parts[0]
    for part in parts[1:]:
        out = out + part
    return out


def body(
    inputs,
    picture_start,
    prenorm_gain,
    prenorm_shift,
    query_weight,
    query_bias,
    key_weight,
    value_weight,
    value_bias,
    output_weight,
    output_bias,
    midnorm_gain,
    midnorm_shift,
    hidden_weight,
    hidden_bias,
    project_weight,
    project_bias,
    cotangent,
    *,
    dp,
    mp,
):
    tokens, width = inputs.shape
    shard = query_weight.shape[1]
    hidden = hidden_weight.shape[1]
    group = HALF // tokens
    me = lax.axis_index("mp")
    groups = [list(range(i, i + group)) for i in range(0, mp, group)]

    def gather(weight):
        whole = lax.all_gather(weight, ("mp", "dp"), axis=0, tiled=True)
        return whole.reshape(mp, width, weight.shape[1])

    def scatter(parts):
        columns = parts[0].shape[1]
        lanes = -columns % 256
        whole = jnp.concatenate([part.astype(BF16) for part in parts], axis=0)
        whole = jnp.pad(whole, ((0, 0), (0, lanes)))
        mine = lax.psum_scatter(whole, ("mp", "dp"), scatter_dimension=0, tiled=True)
        return mine[:, :columns].astype(F32)

    def to_heads(part):
        kinds = part.shape[0]
        if group == 1:
            return part
        part = part.reshape(kinds, group, HEADS // group, HEAD, tokens).transpose(1, 0, 2, 3, 4)
        part = lax.all_to_all(part, "mp", 0, 0, axis_index_groups=groups, tiled=True)
        return part.transpose(1, 2, 3, 0, 4).reshape(kinds, HEADS // group, HEAD, HALF)

    def from_heads(part):
        kinds = part.shape[0]
        if group == 1:
            return part
        part = part.reshape(kinds, HEADS // group, HEAD, group, tokens).transpose(3, 0, 1, 2, 4)
        part = lax.all_to_all(part, "mp", 0, 0, axis_index_groups=groups, tiled=True)
        return part.transpose(1, 0, 2, 3, 4).reshape(kinds, HEADS, HEAD, tokens)

    query_bias_all, value_bias_all, hidden_bias_all = (
        lax.all_gather(item, "mp", axis=0, tiled=False)
        for item in (query_bias, value_bias, hidden_bias)
    )
    half = me // group
    starts = lax.dynamic_slice_in_dim(picture_start, half * HALF, HALF)
    masks = picture_masks(starts)

    attn_weights = gather(jnp.concatenate([query_weight, key_weight, value_weight], axis=1))
    output_all = gather(output_weight.T)
    hidden_all = gather(hidden_weight)
    project_all = gather(project_weight.T)

    residual_in = inputs.astype(F32)
    normed_pre, rstd_pre = local_norm(residual_in)
    attn_in = (normed_pre * prenorm_gain + prenorm_shift).astype(BF16)

    stacks = []
    for j in range(mp):
        bias = jnp.concatenate(
            [query_bias_all[j], jnp.zeros((shard,), F32), value_bias_all[j]], axis=0
        )
        rows = (dot(attn_weights[j], attn_in, 0, 1) + bias[:, None]).astype(BF16)
        stacks.append(rows.reshape(3, shard // HEAD, HEAD, tokens))
    if group == 1:
        pieces = stacks
    else:
        pieces = [to_heads(jnp.concatenate(stacks, axis=1))]
    mixed_pieces, log_pieces, tops = [], [], []
    for piece in pieces:
        mixed_piece, log_piece, top_piece = attention_forward(masks, piece)
        mixed_pieces.append(mixed_piece)
        log_pieces.append(log_piece)
        tops.append(jnp.max(top_piece, axis=(1, 2)))
    peak_here = jnp.concatenate(tops) / LOG2E
    if group == 1:
        mixed = [piece.reshape(shard, tokens) for piece in mixed_pieces]
    else:
        rows = from_heads(mixed_pieces[0][None])[0].reshape(mp, shard, tokens)
        mixed = [rows[j] for j in range(mp)]
        spread = jnp.full((HEADS,), MASKED_SCORE, F32)
        peak_here = lax.dynamic_update_slice_in_dim(
            spread, peak_here, (me % group) * (HEADS // group), 0
        )
    peak_all = lax.pmax(peak_here, ("dp", "mp"))
    logit_peak = lax.dynamic_slice_in_dim(peak_all, me * (HEADS // mp), HEADS // mp)
    factor = jnp.repeat(jnp.sqrt(CLIP_LIMIT / jnp.maximum(logit_peak, CLIP_LIMIT)), HEAD)
    clipped_query = query_weight.astype(F32) * factor[None, :]
    clipped_key = key_weight.astype(F32) * factor[None, :]

    residual_mid = (
        residual_in + total([dot(mixed[j], output_all[j], 0, 1) for j in range(mp)]) + output_bias
    )
    normed_mid, rstd_mid = local_norm(residual_mid)
    mlp_in = (normed_mid * midnorm_gain + midnorm_shift).astype(BF16)
    activated, slopes = [], []
    for j in range(mp):
        value, slope = gelu_parts(dot(mlp_in, hidden_all[j]) + hidden_bias_all[j])
        activated.append(value.astype(BF16))
        slopes.append(slope.astype(BF16))
    project_parts = [dot(cotangent, activated[j], 0, 0) for j in range(mp)]
    project_grad = scatter(project_parts)
    grad_up = [
        (dot(cotangent, project_all[j]) * slopes[j].astype(F32)).astype(BF16) for j in range(mp)
    ]
    hidden_grad = scatter([dot(mlp_in, grad_up[j], 0, 0) for j in range(mp)])
    final_rows = (
        residual_mid
        + total([dot(activated[j], project_all[j], 1, 1) for j in range(mp)])
        + project_bias
    )
    layer_output = final_rows.astype(BF16)

    grad_output = cotangent.astype(F32)
    grad_mid = total([dot(grad_up[j], hidden_all[j], 1, 1) for j in range(mp)])
    grad_resid = grad_output + norm_backward(grad_mid, normed_mid, rstd_mid, midnorm_gain)
    grad_branch = grad_resid.astype(BF16)
    output_grad = scatter([dot(grad_branch, mixed[j], 0, 1) for j in range(mp)])
    grad_mixed = [
        dot(output_all[j], grad_branch, 0, 1).astype(BF16).reshape(shard // HEAD, HEAD, tokens)
        for j in range(mp)
    ]
    if group > 1:
        grad_mixed = [to_heads(jnp.concatenate(grad_mixed, axis=0)[None])[0]]
    grad_pieces = [
        attention_backward(masks, piece, mixed_piece, log_piece, grads)
        for piece, mixed_piece, log_piece, grads in zip(
            pieces, mixed_pieces, log_pieces, grad_mixed
        )
    ]
    if group > 1:
        whole = from_heads(grad_pieces[0]).reshape(3, mp, shard // HEAD, HEAD, tokens)
        grad_pieces = [whole[:, j] for j in range(mp)]
    grad_rows = [piece.reshape(3 * shard, tokens) for piece in grad_pieces]
    attn_grad = scatter([dot(attn_in, grad_rows[j], 0, 1) for j in range(mp)])
    grad_pre = total([dot(grad_rows[j], attn_weights[j], 0, 1) for j in range(mp)])
    inputs_gradient = grad_resid + norm_backward(grad_pre, normed_pre, rstd_pre, prenorm_gain)

    row_sums = [jnp.sum(rows.astype(F32), axis=1) for rows in grad_rows]
    head_parts = (
        jnp.stack([sums[:shard] for sums in row_sums]),
        jnp.stack([sums[2 * shard :] for sums in row_sums]),
        jnp.stack([jnp.sum(part.astype(F32), axis=0) for part in grad_up]),
    )
    norm_parts = (
        jnp.sum(grad_pre * normed_pre, axis=0),
        jnp.sum(grad_pre, axis=0),
        jnp.sum(grad_branch.astype(F32), axis=0),
        jnp.sum(grad_mid * normed_mid, axis=0),
        jnp.sum(grad_mid, axis=0),
        jnp.sum(grad_output, axis=0),
    )
    flat = jnp.concatenate([item.reshape(-1) for item in (*head_parts, *norm_parts)])
    flat = lax.psum(flat, ("dp", "mp"))
    ends = [mp * shard, mp * shard, mp * hidden] + [width] * 6
    sums, at = [], 0
    for size in ends:
        sums.append(flat[at : at + size])
        at += size
    query_bias_grad, value_bias_grad, hidden_bias_grad = (
        lax.dynamic_index_in_dim(item.reshape(mp, -1), me, keepdims=False) for item in sums[:3]
    )
    return (
        layer_output,
        inputs_gradient,
        sums[3],
        sums[4],
        attn_grad[:, :shard],
        query_bias_grad,
        attn_grad[:, shard : 2 * shard],
        attn_grad[:, 2 * shard :],
        value_bias_grad,
        output_grad.T,
        sums[5],
        sums[6],
        sums[7],
        hidden_grad,
        hidden_bias_grad,
        project_grad.T,
        sums[8],
        logit_peak,
        clipped_query,
        clipped_key,
    )


def solution(mesh):
    rows = P(("dp", "mp"), None)
    split = P("dp", "mp")
    turned = P("mp", "dp")
    heads = P("mp")
    whole = P()
    placed = (
        rows, P("dp"), whole, whole, split, heads, split, split, heads, turned, whole, whole, whole,
        split, heads, turned, whole, rows,
    )
    given = (
        rows, rows, whole, whole, split, heads, split, split, heads, turned, whole, whole, whole,
        split, heads, turned, whole, heads, split, split,
    )
    return jax.shard_map(
        partial(body, dp=mesh.shape["dp"], mp=mesh.shape["mp"]),
        mesh=mesh,
        in_specs=placed,
        out_specs=given,
        check_vma=False,
    )
```

```python
import math
from functools import partial

import jax
import jax.numpy as jnp
from jax import lax
from jax.experimental import pallas as pl
from jax.experimental.pallas import tpu as pltpu
from jax.sharding import PartitionSpec as P

HEAD = 72
HEADS = 16
ROW = 2048
HALF = 1024
EPSILON = 1e-06
CLIP_LIMIT = 7.0
MASKED_SCORE = -1e30
FEATURES = 16
PICTURES = 10
QUERY_BLOCK = 256
SCALE = HEAD ** (-0.5)
LOG2E = 1.0 / math.log(2.0)
EXPONENT = SCALE * LOG2E
F32 = jnp.float32
BF16 = jnp.bfloat16


def dot(left, right, left_dim=1, right_dim=0):
    return lax.dot_general(
        left, right, (((left_dim,), (right_dim,)), ((), ())), preferred_element_type=F32
    )


def split_terms(value, count):
    terms = []
    for _ in range(count):
        term = value.astype(BF16).astype(F32)
        terms.append(term)
        value = value - term
    return terms


def query_operand(query, features):
    pad = jnp.zeros((8, query.shape[1]), F32)
    high, low = split_terms(query.astype(F32) * EXPONENT, 2)
    return jnp.concatenate([high, pad, low, pad, features], axis=0).astype(BF16)


def key_operand(key, features):
    pad = jnp.zeros((8, key.shape[1]), F32)
    wide = key.astype(F32)
    stacked = jnp.concatenate([wide, pad, wide, pad, features], axis=0)
    return stacked.T.astype(BF16)


def rows_below(wide, extra):
    width = wide.shape[1]
    row = lax.broadcasted_iota(jnp.int32, (8, width), 0)
    block = jnp.zeros((8, width), F32)
    for position, line in enumerate(extra):
        block = jnp.where(row == position, line, block)
    return jnp.concatenate([wide, block], axis=0)


def forward_kernel(mask_ref, key_mask_ref, query_ref, key_ref, value_ref, mixed_ref, log_ref, top_ref):
    query_rows = query_operand(query_ref[0, 0], mask_ref[...])
    key_rows = key_operand(key_ref[0, 0], key_mask_ref[...])
    value_rows = rows_below(value_ref[0, 0].astype(F32), [jnp.ones((1, 1), F32)]).astype(BF16)
    for begin in range(0, HALF, QUERY_BLOCK):
        block = slice(begin, begin + QUERY_BLOCK)
        scores = dot(key_rows, query_rows[:, block])
        top = jnp.max(scores, axis=0, keepdims=True)
        weights = jnp.exp2(scores - top).astype(BF16)
        summed = dot(value_rows, weights)
        total = summed[HEAD : HEAD + 1]
        mixed_ref[0, :, block] = (summed[:HEAD] / total).astype(BF16)
        log_ref[0, :, block] = top + jnp.log2(total)
        top_ref[0, :, block] = top


def backward_kernel(
    mask_ref, key_mask_ref, query_ref, key_ref, value_ref, mixed_ref, log_ref, grad_ref, out_ref
):
    query, key = query_ref[0, 0], key_ref[0, 0]
    grad = grad_ref[0]
    row = lax.broadcasted_iota(jnp.int32, (FEATURES, HALF), 0)
    features = mask_ref[...]
    for position, term in enumerate(split_terms(-log_ref[0], 3)):
        features = jnp.where(row == PICTURES + position, term, features)
    query_rows = query_operand(query, features)
    key_rows = key_operand(key, key_mask_ref[...])
    grad_wide = grad.astype(F32)
    delta = jnp.sum(grad_wide * mixed_ref[0].astype(F32), axis=0, keepdims=True)
    grad_rows = rows_below(grad_wide, split_terms(-delta, 2)).astype(BF16)
    one = jnp.ones((1, 1), F32)
    value_rows = rows_below(value_ref[0, 0].astype(F32), [one, one]).T.astype(BF16)
    query_cols = query.astype(F32).T.astype(BF16)
    grad_cols = grad_wide.T.astype(BF16)
    grad_key = jnp.zeros((HALF, HEAD), F32)
    grad_value = jnp.zeros((HALF, HEAD), F32)
    for begin in range(0, HALF, QUERY_BLOCK):
        block = slice(begin, begin + QUERY_BLOCK)
        weights = jnp.exp2(dot(key_rows, query_rows[:, block]))
        slopes = dot(value_rows, grad_rows[:, block])
        grad_scores = (weights * slopes).astype(BF16)
        grad_value = grad_value + dot(weights.astype(BF16), grad_cols[block])
        grad_key = grad_key + dot(grad_scores, query_cols[block])
        out_ref[0, 0, :, block] = (dot(key, grad_scores) * SCALE).astype(BF16)
    out_ref[1, 0] = (grad_key * SCALE).T.astype(BF16)
    out_ref[2, 0] = grad_value.T.astype(BF16)


def head_specs():
    features = pl.BlockSpec((FEATURES, HALF), lambda h: (0, 0))
    part = [pl.BlockSpec((1, 1, HEAD, HALF), lambda h, i=i: (i, h, 0, 0)) for i in range(3)]
    head = pl.BlockSpec((1, HEAD, HALF), lambda h: (h, 0, 0))
    line = pl.BlockSpec((1, 1, HALF), lambda h: (h, 0, 0))
    return features, part, head, line


def attention_forward(masks, stacked):
    heads = stacked.shape[1]
    features, part, head, line = head_specs()
    area = heads * HALF * HALF
    return pl.pallas_call(
        forward_kernel,
        grid=(heads,),
        in_specs=[features, features, *part],
        out_specs=(head, line, line),
        out_shape=(
            jax.ShapeDtypeStruct((heads, HEAD, HALF), BF16),
            jax.ShapeDtypeStruct((heads, 1, HALF), F32),
            jax.ShapeDtypeStruct((heads, 1, HALF), F32),
        ),
        cost_estimate=pl.CostEstimate(
            flops=area * 2 * 256 * 2, bytes_accessed=heads * HALF * HEAD * 8, transcendentals=area
        ),
        name="attention_forward",
    )(*masks, stacked, stacked, stacked)


def attention_backward(masks, stacked, mixed, logs, grads):
    heads = stacked.shape[1]
    features, part, head, line = head_specs()
    area = heads * HALF * HALF
    return pl.pallas_call(
        backward_kernel,
        grid=(heads,),
        in_specs=[features, features, *part, head, line, head],
        out_specs=pl.BlockSpec((3, 1, HEAD, HALF), lambda h: (0, h, 0, 0)),
        out_shape=jax.ShapeDtypeStruct((3, heads, HEAD, HALF), BF16),
        cost_estimate=pl.CostEstimate(
            flops=area * 2 * 256 * 5, bytes_accessed=heads * HALF * HEAD * 16, transcendentals=area
        ),
        name="attention_backward",
    )(*masks, stacked, stacked, stacked, mixed, logs, grads)


def picture_masks(starts):
    before = jnp.concatenate([starts[:1], starts[:-1]])
    changes = (starts != before).astype(F32)
    place = lax.iota(jnp.int32, HALF)
    number = jnp.sum(jnp.where(place[:, None] <= place[None, :], changes[:, None], 0.0), axis=0)
    row = lax.broadcasted_iota(jnp.int32, (FEATURES, HALF), 0)
    same = row.astype(F32) == number[None, :]
    listed = row < PICTURES
    mask = jnp.where(listed & ~same, MASKED_SCORE, 0.0)
    key_mask = jnp.where(listed, same.astype(F32), (row < PICTURES + 3).astype(F32))
    return mask, key_mask


LINE = 4
SEAM = 40
MESH = pl.DeviceIdType.MESH


def place_of():
    at, y = lax.axis_index("dp"), lax.axis_index("mp")
    return at // 4, (at // 2) % 2, y, at % 2


def device_of(z, x, y, core):
    return ((z * 2 + x) * 2 + core, y)


def neighbours(z, x, y, core):
    return (
        device_of(z, x, y, 1 - core), device_of(z, 1 - x, y, core), device_of(z, x, 1 - y, core)
    )


def enter(z, x, y, core):
    barrier = pltpu.get_barrier_semaphore()
    for device in neighbours(z, x, y, core):
        pl.semaphore_signal(barrier, inc=1, device_id=device, device_id_type=MESH)

    @pl.when(z > 0)
    def _():
        pl.semaphore_signal(barrier, inc=1, device_id=device_of(z - 1, x, y, core), device_id_type=MESH)

    @pl.when(z < LINE - 1)
    def _():
        pl.semaphore_signal(barrier, inc=1, device_id=device_of(z + 1, x, y, core), device_id_type=MESH)

    pl.semaphore_wait(barrier, 3 + jnp.where(z > 0, 1, 0) + jnp.where(z < LINE - 1, 1, 0))


def gather_kernel(count, *refs):
    shards, wholes = refs[:count], refs[count : 2 * count]
    own_sem, z_send, z_recv, side_send, side_recv, core_send, core_recv = refs[2 * count :]
    z, x, y, core = place_of()
    rows = shards[0].shape[0]
    parts = (pl.ds(0, SEAM), pl.ds(SEAM, rows - SEAM))
    other, across_x, across_y = neighbours(z, x, y, core)

    def spot(a, zz, xx, yy, part=None):
        view = wholes[a].at[yy, (zz * 2 + xx) * 2 + core]
        return view if part is None else view.at[parts[part]]

    def along_z(a, zz, upward, source):
        return pltpu.make_async_remote_copy(
            spot(a, zz, x, y), spot(a, zz, x, y),
            z_send.at[a, zz, 1 if upward else 0], z_recv.at[a, zz],
            device_of(source + (1 if upward else -1), x, y, core), MESH,
        )

    def sideways(a, half, stage, zz, flip):
        first = half == 0
        over_x = first == (stage == 0)
        xx = x if over_x else (1 - x if flip else x)
        yy = y if not over_x else (1 - y if flip else y)
        block = spot(a, zz, xx, yy, half)
        slot = zz * 2 + (1 if flip else 0)
        return pltpu.make_async_remote_copy(
            block, block, side_send.at[a, half, stage, slot], side_recv.at[a, half, stage, slot],
            across_x if over_x else across_y, MESH,
        )

    def arrival(a, half, stage, zz, flip):
        first = half == 0
        over_x = first == (stage == 0)
        xx = 1 - x if over_x else (1 - x if flip else x)
        yy = 1 - y if not over_x else (1 - y if flip else y)
        block = spot(a, zz, xx, yy, half)
        slot = zz * 2 + (1 if flip else 0)
        return pltpu.make_async_remote_copy(
            block, block, side_send.at[a, half, stage, slot], side_recv.at[a, half, stage, slot],
            across_x if over_x else across_y, MESH,
        )

    def hand_over(a, half, zz, fx, fy):
        xx = 1 - x if fx else x
        yy = 1 - y if fy else y
        block = spot(a, zz, xx, yy, half)
        slot = zz * 4 + (2 if fx else 0) + (1 if fy else 0)
        return pltpu.make_async_remote_copy(
            block, block, core_send.at[a, half, slot], core_recv.at[a, half, slot], other, MESH
        )

    def handed(a, half, zz, fx, fy):
        xx = 1 - x if fx else x
        yy = 1 - y if fy else y
        block = wholes[a].at[yy, (zz * 2 + xx) * 2 + 1 - core].at[parts[half]]
        slot = zz * 4 + (2 if fx else 0) + (1 if fy else 0)
        return pltpu.make_async_remote_copy(
            block, block, core_send.at[a, half, slot], core_recv.at[a, half, slot], other, MESH
        )

    def launch_line_block(a, zz):
        for half in range(2):
            sideways(a, half, 0, zz, False).start()
            sideways(a, half, 1, zz, False).start()
            hand_over(a, half, zz, False, False).start()

    def stage_begin(a):
        own = pltpu.make_async_copy(shards[a], spot(a, z, x, y), own_sem.at[a])
        own.start()
        own.wait()

        @pl.when(z < LINE - 1)
        def _():
            along_z(a, z, True, z).start()

        @pl.when(z > 0)
        def _():
            along_z(a, z, False, z).start()

        launch_line_block(a, z)

    def stage_hop(a, hop):
        @pl.when(z >= hop)
        def _():
            origin = z - hop
            along_z(a, origin, True, z - 1).wait_recv()

            @pl.when(z < LINE - 1)
            def _():
                along_z(a, origin, True, z).start()

            launch_line_block(a, origin)

        @pl.when(z < LINE - hop)
        def _():
            origin = z + hop
            along_z(a, origin, False, z + 1).wait_recv()

            @pl.when(z > 0)
            def _():
                along_z(a, origin, False, z).start()

            launch_line_block(a, origin)

    def stage_turn(a):
        for zz in range(LINE):
            for half in range(2):
                arrival(a, half, 0, zz, False).wait_recv()
                sideways(a, half, 1, zz, True).start()
                hand_over(a, half, zz, half == 0, half == 1).start()

    def stage_last(a):
        for zz in range(LINE):
            for half in range(2):
                arrival(a, half, 1, zz, False).wait_recv()
                hand_over(a, half, zz, half == 1, half == 0).start()
                arrival(a, half, 1, zz, True).wait_recv()
                hand_over(a, half, zz, True, True).start()

    def stage_close(a):
        for zz in range(LINE):
            for half in range(2):
                for fx in (False, True):
                    for fy in (False, True):
                        handed(a, half, zz, fx, fy).wait_recv()
                        hand_over(a, half, zz, fx, fy).wait_send()
                sideways(a, half, 0, zz, False).wait_send()
                sideways(a, half, 1, zz, False).wait_send()
                sideways(a, half, 1, zz, True).wait_send()

            @pl.when(jnp.logical_and(z >= zz, z < LINE - 1))
            def _():
                along_z(a, zz, True, z).wait_send()

            @pl.when(jnp.logical_and(z <= zz, z > 0))
            def _():
                along_z(a, zz, False, z).wait_send()

    enter(z, x, y, core)
    stages = [
        stage_begin, partial(stage_hop, hop=1), partial(stage_hop, hop=2), partial(stage_hop, hop=3),
        stage_turn, stage_last, stage_close,
    ]
    for step in range(len(stages) + count - 1):
        for a in range(count):
            if 0 <= step - a < len(stages):
                stages[step - a](a)


def gather_blocks(shards, mp):
    count, rows = len(shards), shards[0].shape[0]
    dp = 16
    anywhere = pl.BlockSpec(memory_space=pl.ANY)
    dma = pltpu.SemaphoreType.DMA
    sent = sum(item.size * 2 for item in shards) * 15
    wholes = pl.pallas_call(
        partial(gather_kernel, count),
        in_specs=[anywhere] * count,
        out_specs=[anywhere] * count,
        out_shape=[jax.ShapeDtypeStruct((mp, dp, rows, item.shape[1]), BF16) for item in shards],
        scratch_shapes=[
            dma((count,)), dma((count, LINE, 2)), dma((count, LINE)), dma((count, 2, 2, 8)),
            dma((count, 2, 2, 8)), dma((count, 2, 16)), dma((count, 2, 16)),
        ],
        compiler_params=pltpu.CompilerParams(collective_id=0, has_side_effects=True),
        cost_estimate=pl.CostEstimate(flops=0, bytes_accessed=sent, transcendentals=0),
        name="gather_blocks",
    )(*shards)
    return [whole.reshape(mp, dp * rows, whole.shape[-1]) for whole in wholes]


def gradient_kernel(count, left_ref, *refs):
    rights, out_ref = refs[:count], refs[count]
    columns = rights[0].shape[0]
    for j in range(count):

        @pl.when(pl.program_id(0) == j)
        def _():
            out_ref[0, :, :columns] = dot(left_ref[...], rights[j][...], 1, 1).astype(BF16)

    if columns < out_ref.shape[2]:
        extra = out_ref.shape[2] - columns
        out_ref[0, :, columns:] = jnp.zeros((out_ref.shape[1], extra), BF16)


def weight_gradient(left, rights, lanes):
    width, tokens = left.shape
    count, columns = len(rights), rights[0].shape[0]
    padded = columns + -columns % lanes
    tile = 384
    whole = lambda j, m: (0, 0)
    return pl.pallas_call(
        partial(gradient_kernel, count),
        grid=(count, width // tile),
        in_specs=[pl.BlockSpec((tile, tokens), lambda j, m: (m, 0))]
        + [pl.BlockSpec((columns, tokens), whole)] * count,
        out_specs=pl.BlockSpec((1, tile, padded), lambda j, m: (j, m, 0)),
        out_shape=jax.ShapeDtypeStruct((count, width, padded), BF16),
        cost_estimate=pl.CostEstimate(
            flops=2 * width * tokens * columns * count,
            bytes_accessed=2 * count * (width * padded + columns * tokens) + 2 * width * tokens,
            transcendentals=0,
        ),
        name="weight_gradient",
    )(left, *rights)


def local_norm(values):
    centre = jnp.mean(values, axis=1, keepdims=True)
    centred = values - centre
    rstd = lax.rsqrt(jnp.mean(centred * centred, axis=1, keepdims=True) + EPSILON)
    return centred * rstd, rstd


def norm_backward(grad_normed, normed, rstd, gain):
    scaled = grad_normed * gain
    mean_grad = jnp.mean(scaled, axis=1, keepdims=True)
    mean_cross = jnp.mean(scaled * normed, axis=1, keepdims=True)
    return rstd * (scaled - mean_grad - normed * mean_cross)


def gelu_parts(rows):
    cubic = math.sqrt(2.0 / math.pi) * (rows + 0.044715 * rows * rows * rows)
    bend = jnp.tanh(cubic)
    value = 0.5 * rows * (1.0 + bend)
    slope = 0.5 * (1.0 + bend) + 0.5 * rows * (1.0 - bend * bend) * (
        math.sqrt(2.0 / math.pi) * (1.0 + 3.0 * 0.044715 * rows * rows)
    )
    return value, slope


def total(parts):
    out = parts[0]
    for part in parts[1:]:
        out = out + part
    return out


def body(
    inputs,
    picture_start,
    prenorm_gain,
    prenorm_shift,
    query_weight,
    query_bias,
    key_weight,
    value_weight,
    value_bias,
    output_weight,
    output_bias,
    midnorm_gain,
    midnorm_shift,
    hidden_weight,
    hidden_bias,
    project_weight,
    project_bias,
    cotangent,
    *,
    dp,
    mp,
):
    tokens, width = inputs.shape
    shard = query_weight.shape[1]
    hidden = hidden_weight.shape[1]
    group = HALF // tokens
    me = lax.axis_index("mp")
    groups = [list(range(i, i + group)) for i in range(0, mp, group)]

    fitted = dp == 16 and mp == 2
    lanes = 256

    def gather(weight):
        whole = lax.all_gather(weight, ("mp", "dp"), axis=0, tiled=True)
        return whole.reshape(mp, width, weight.shape[1])

    def scatter(parts, columns):
        whole = parts.reshape(mp * width, parts.shape[2])
        mine = lax.psum_scatter(whole, ("mp", "dp"), scatter_dimension=0, tiled=True)
        return lax.optimization_barrier(mine)[:, :columns].astype(F32)

    def to_heads(part):
        kinds = part.shape[0]
        if group == 1:
            return part
        part = part.reshape(kinds, group, HEADS // group, HEAD, tokens).transpose(1, 0, 2, 3, 4)
        part = lax.all_to_all(part, "mp", 0, 0, axis_index_groups=groups, tiled=True)
        return part.transpose(1, 2, 3, 0, 4).reshape(kinds, HEADS // group, HEAD, HALF)

    def from_heads(part):
        kinds = part.shape[0]
        if group == 1:
            return part
        part = part.reshape(kinds, HEADS // group, HEAD, group, tokens).transpose(3, 0, 1, 2, 4)
        part = lax.all_to_all(part, "mp", 0, 0, axis_index_groups=groups, tiled=True)
        return part.transpose(1, 0, 2, 3, 4).reshape(kinds, HEADS, HEAD, tokens)

    query_bias_all, value_bias_all, hidden_bias_all = (
        lax.all_gather(item, "mp", axis=0, tiled=False)
        for item in (query_bias, value_bias, hidden_bias)
    )
    half = me // group
    starts = lax.dynamic_slice_in_dim(picture_start, half * HALF, HALF)
    masks = picture_masks(starts)

    attn_shard = jnp.concatenate([query_weight, key_weight, value_weight], axis=1)
    if fitted:
        attn_weights, output_all = gather_blocks([attn_shard, output_weight.T], mp)
        attn_weights, hidden_shard, project_shard = lax.optimization_barrier(
            (attn_weights, hidden_weight, project_weight)
        )
    else:
        attn_weights, output_all = gather(attn_shard), gather(output_weight.T)
        hidden_shard, project_shard = hidden_weight, project_weight
    hidden_all = gather(hidden_shard)
    project_all = gather(project_shard.T)

    residual_in = inputs.astype(F32)
    normed_pre, rstd_pre = local_norm(residual_in)
    attn_in = (normed_pre * prenorm_gain + prenorm_shift).astype(BF16)

    stacks = []
    for j in range(mp):
        bias = jnp.concatenate(
            [query_bias_all[j], jnp.zeros((shard,), F32), value_bias_all[j]], axis=0
        )
        rows = (dot(attn_weights[j], attn_in, 0, 1) + bias[:, None]).astype(BF16)
        stacks.append(rows.reshape(3, shard // HEAD, HEAD, tokens))
    if group == 1:
        pieces = stacks
    else:
        pieces = [to_heads(jnp.concatenate(stacks, axis=1))]
    mixed_pieces, log_pieces, tops = [], [], []
    for piece in pieces:
        mixed_piece, log_piece, top_piece = attention_forward(masks, piece)
        mixed_pieces.append(mixed_piece)
        log_pieces.append(log_piece)
        tops.append(jnp.max(top_piece, axis=(1, 2)))
    peak_here = jnp.concatenate(tops) / LOG2E
    if group == 1:
        mixed = [piece.reshape(shard, tokens) for piece in mixed_pieces]
    else:
        rows = from_heads(mixed_pieces[0][None])[0].reshape(mp, shard, tokens)
        mixed = [rows[j] for j in range(mp)]
        spread = jnp.full((HEADS,), MASKED_SCORE, F32)
        peak_here = lax.dynamic_update_slice_in_dim(
            spread, peak_here, (me % group) * (HEADS // group), 0
        )
    residual_mid = (
        residual_in + total([dot(mixed[j], output_all[j], 0, 1) for j in range(mp)]) + output_bias
    )
    normed_mid, rstd_mid = local_norm(residual_mid)
    mlp_in = (normed_mid * midnorm_gain + midnorm_shift).astype(BF16)
    activated, slopes = [], []
    for j in range(mp):
        value, slope = gelu_parts(dot(hidden_all[j], mlp_in, 0, 1) + hidden_bias_all[j][:, None])
        activated.append(value.astype(BF16))
        slopes.append(slope.astype(BF16))
    activated, slopes = lax.optimization_barrier((activated, slopes))
    project_parts = weight_gradient(cotangent.T, activated, lanes)
    project_parts, late_cotangent = lax.optimization_barrier((project_parts, cotangent))
    project_grad = scatter(project_parts, hidden)
    grad_up = [
        (dot(project_all[j], late_cotangent, 0, 1) * slopes[j].astype(F32)).astype(BF16)
        for j in range(mp)
    ]
    grad_up = lax.optimization_barrier(grad_up)
    hidden_parts = weight_gradient(mlp_in.T, grad_up, lanes)
    hidden_parts, grad_up, activated = lax.optimization_barrier((hidden_parts, grad_up, activated))
    hidden_grad = scatter(hidden_parts, hidden)
    final_rows = (
        residual_mid
        + total([dot(activated[j], project_all[j], 0, 1) for j in range(mp)])
        + project_bias
    )
    layer_output = final_rows.astype(BF16)

    grad_output = cotangent.astype(F32)
    grad_mid = total([dot(grad_up[j], hidden_all[j], 0, 1) for j in range(mp)])
    grad_resid = grad_output + norm_backward(grad_mid, normed_mid, rstd_mid, midnorm_gain)
    grad_branch = grad_resid.astype(BF16)
    output_grad = scatter(weight_gradient(grad_branch.T, mixed, lanes), shard)
    grad_mixed = [
        dot(output_all[j], grad_branch, 0, 1).astype(BF16).reshape(shard // HEAD, HEAD, tokens)
        for j in range(mp)
    ]
    if group > 1:
        grad_mixed = [to_heads(jnp.concatenate(grad_mixed, axis=0)[None])[0]]
    grad_pieces = [
        attention_backward(masks, piece, mixed_piece, log_piece, grads)
        for piece, mixed_piece, log_piece, grads in zip(
            pieces, mixed_pieces, log_pieces, grad_mixed
        )
    ]
    if group > 1:
        whole = from_heads(grad_pieces[0]).reshape(3, mp, shard // HEAD, HEAD, tokens)
        grad_pieces = [whole[:, j] for j in range(mp)]
    grad_rows = [piece.reshape(3 * shard, tokens) for piece in grad_pieces]
    attn_grad = scatter(weight_gradient(attn_in.T, grad_rows, lanes), 3 * shard)
    grad_pre = total([dot(grad_rows[j], attn_weights[j], 0, 1) for j in range(mp)])
    inputs_gradient = grad_resid + norm_backward(grad_pre, normed_pre, rstd_pre, prenorm_gain)

    row_sums = [jnp.sum(rows.astype(F32), axis=1) for rows in grad_rows]
    head_parts = (
        jnp.stack([sums[:shard] for sums in row_sums]),
        jnp.stack([sums[2 * shard :] for sums in row_sums]),
        jnp.stack([jnp.sum(part.astype(F32), axis=1) for part in grad_up]),
    )
    norm_parts = (
        jnp.sum(grad_pre * normed_pre, axis=0),
        jnp.sum(grad_pre, axis=0),
        jnp.sum(grad_branch.astype(F32), axis=0),
        jnp.sum(grad_mid * normed_mid, axis=0),
        jnp.sum(grad_mid, axis=0),
        jnp.sum(grad_output, axis=0),
    )
    slot = lax.axis_index("dp") * mp + me
    peak_slots = jnp.where(lax.iota(jnp.int32, dp * mp)[:, None] == slot, peak_here[None, :], 0.0)
    flat = jnp.concatenate([item.reshape(-1) for item in (*head_parts, *norm_parts, peak_slots)])
    flat = lax.psum(flat, ("dp", "mp"))
    ends = [mp * shard, mp * shard, mp * hidden] + [width] * 6
    sums, at = [], 0
    for size in ends:
        sums.append(flat[at : at + size])
        at += size
    peak_all = jnp.max(flat[at:].reshape(dp * mp, HEADS), axis=0)
    logit_peak = lax.dynamic_slice_in_dim(peak_all, me * (HEADS // mp), HEADS // mp)
    factor = jnp.repeat(jnp.sqrt(CLIP_LIMIT / jnp.maximum(logit_peak, CLIP_LIMIT)), HEAD)
    clipped_query = query_weight.astype(F32) * factor[None, :]
    clipped_key = key_weight.astype(F32) * factor[None, :]
    query_bias_grad, value_bias_grad, hidden_bias_grad = (
        lax.dynamic_index_in_dim(item.reshape(mp, -1), me, keepdims=False) for item in sums[:3]
    )
    return (
        layer_output,
        inputs_gradient,
        sums[3],
        sums[4],
        attn_grad[:, :shard],
        query_bias_grad,
        attn_grad[:, shard : 2 * shard],
        attn_grad[:, 2 * shard :],
        value_bias_grad,
        output_grad.T,
        sums[5],
        sums[6],
        sums[7],
        hidden_grad,
        hidden_bias_grad,
        project_grad.T,
        sums[8],
        logit_peak,
        clipped_query,
        clipped_key,
    )


def solution(mesh):
    rows = P(("dp", "mp"), None)
    split = P("dp", "mp")
    turned = P("mp", "dp")
    heads = P("mp")
    whole = P()
    placed = (
        rows, P("dp"), whole, whole, split, heads, split, split, heads, turned, whole, whole, whole,
        split, heads, turned, whole, rows,
    )
    given = (
        rows, rows, whole, whole, split, heads, split, split, heads, turned, whole, whole, whole,
        split, heads, turned, whole, heads, split, split,
    )
    return jax.shard_map(
        partial(body, dp=mesh.shape["dp"], mp=mesh.shape["mp"]),
        mesh=mesh,
        in_specs=placed,
        out_specs=given,
        check_vma=False,
    )
```

```python
import math
from functools import partial

import jax
import jax.numpy as jnp
from jax import lax
from jax.experimental import pallas as pl
from jax.experimental.pallas import tpu as pltpu
from jax.sharding import PartitionSpec as P

HEAD = 72
HEADS = 16
ROW = 2048
HALF = 1024
EPSILON = 1e-06
CLIP_LIMIT = 7.0
MASKED_SCORE = -1e30
FEATURES = 16
PICTURES = 10
QUERY_BLOCK = 256
SCALE = HEAD ** (-0.5)
LOG2E = 1.0 / math.log(2.0)
EXPONENT = SCALE * LOG2E
F32 = jnp.float32
BF16 = jnp.bfloat16


def dot(left, right, left_dim=1, right_dim=0):
    return lax.dot_general(
        left, right, (((left_dim,), (right_dim,)), ((), ())), preferred_element_type=F32
    )


def split_terms(value, count):
    terms = []
    for _ in range(count):
        term = value.astype(BF16).astype(F32)
        terms.append(term)
        value = value - term
    return terms


def query_operand(query, features):
    pad = jnp.zeros((8, query.shape[1]), F32)
    high, low = split_terms(query.astype(F32) * EXPONENT, 2)
    return jnp.concatenate([high, pad, low, pad, features], axis=0).astype(BF16)


def key_operand(key, features):
    pad = jnp.zeros((8, key.shape[1]), F32)
    wide = key.astype(F32)
    stacked = jnp.concatenate([wide, pad, wide, pad, features], axis=0)
    return stacked.T.astype(BF16)


def rows_below(wide, extra):
    width = wide.shape[1]
    row = lax.broadcasted_iota(jnp.int32, (8, width), 0)
    block = jnp.zeros((8, width), F32)
    for position, line in enumerate(extra):
        block = jnp.where(row == position, line, block)
    return jnp.concatenate([wide, block], axis=0)


def forward_kernel(mask_ref, key_mask_ref, query_ref, key_ref, value_ref, mixed_ref, log_ref, top_ref):
    query_rows = query_operand(query_ref[0, 0], mask_ref[...])
    key_rows = key_operand(key_ref[0, 0], key_mask_ref[...])
    value_rows = rows_below(value_ref[0, 0].astype(F32), [jnp.ones((1, 1), F32)]).astype(BF16)
    for begin in range(0, HALF, QUERY_BLOCK):
        block = slice(begin, begin + QUERY_BLOCK)
        scores = dot(key_rows, query_rows[:, block])
        top = jnp.max(scores, axis=0, keepdims=True)
        weights = jnp.exp2(scores - top).astype(BF16)
        summed = dot(value_rows, weights)
        total = summed[HEAD : HEAD + 1]
        mixed_ref[0, :, block] = (summed[:HEAD] / total).astype(BF16)
        log_ref[0, :, block] = top + jnp.log2(total)
        top_ref[0, :, block] = top


def backward_kernel(
    mask_ref, key_mask_ref, query_ref, key_ref, value_ref, mixed_ref, log_ref, grad_ref, out_ref
):
    query, key = query_ref[0, 0], key_ref[0, 0]
    grad = grad_ref[0]
    row = lax.broadcasted_iota(jnp.int32, (FEATURES, HALF), 0)
    features = mask_ref[...]
    for position, term in enumerate(split_terms(-log_ref[0], 3)):
        features = jnp.where(row == PICTURES + position, term, features)
    query_rows = query_operand(query, features)
    key_rows = key_operand(key, key_mask_ref[...])
    grad_wide = grad.astype(F32)
    delta = jnp.sum(grad_wide * mixed_ref[0].astype(F32), axis=0, keepdims=True)
    grad_rows = rows_below(grad_wide, split_terms(-delta, 2)).astype(BF16)
    one = jnp.ones((1, 1), F32)
    value_rows = rows_below(value_ref[0, 0].astype(F32), [one, one]).T.astype(BF16)
    query_cols = query.astype(F32).T.astype(BF16)
    grad_cols = grad_wide.T.astype(BF16)
    grad_key = jnp.zeros((HALF, HEAD), F32)
    grad_value = jnp.zeros((HALF, HEAD), F32)
    for begin in range(0, HALF, QUERY_BLOCK):
        block = slice(begin, begin + QUERY_BLOCK)
        weights = jnp.exp2(dot(key_rows, query_rows[:, block]))
        slopes = dot(value_rows, grad_rows[:, block])
        grad_scores = (weights * slopes).astype(BF16)
        grad_value = grad_value + dot(weights.astype(BF16), grad_cols[block])
        grad_key = grad_key + dot(grad_scores, query_cols[block])
        out_ref[0, 0, :, block] = (dot(key, grad_scores) * SCALE).astype(BF16)
    out_ref[1, 0] = (grad_key * SCALE).T.astype(BF16)
    out_ref[2, 0] = grad_value.T.astype(BF16)


def head_specs():
    features = pl.BlockSpec((FEATURES, HALF), lambda h: (0, 0))
    part = [pl.BlockSpec((1, 1, HEAD, HALF), lambda h, i=i: (i, h, 0, 0)) for i in range(3)]
    head = pl.BlockSpec((1, HEAD, HALF), lambda h: (h, 0, 0))
    line = pl.BlockSpec((1, 1, HALF), lambda h: (h, 0, 0))
    return features, part, head, line


def attention_forward(masks, stacked):
    heads = stacked.shape[1]
    features, part, head, line = head_specs()
    area = heads * HALF * HALF
    return pl.pallas_call(
        forward_kernel,
        grid=(heads,),
        in_specs=[features, features, *part],
        out_specs=(head, line, line),
        out_shape=(
            jax.ShapeDtypeStruct((heads, HEAD, HALF), BF16),
            jax.ShapeDtypeStruct((heads, 1, HALF), F32),
            jax.ShapeDtypeStruct((heads, 1, HALF), F32),
        ),
        cost_estimate=pl.CostEstimate(
            flops=area * 2 * 256 * 2, bytes_accessed=heads * HALF * HEAD * 8, transcendentals=area
        ),
        name="attention_forward",
    )(*masks, stacked, stacked, stacked)


def attention_backward(masks, stacked, mixed, logs, grads):
    heads = stacked.shape[1]
    features, part, head, line = head_specs()
    area = heads * HALF * HALF
    return pl.pallas_call(
        backward_kernel,
        grid=(heads,),
        in_specs=[features, features, *part, head, line, head],
        out_specs=pl.BlockSpec((3, 1, HEAD, HALF), lambda h: (0, h, 0, 0)),
        out_shape=jax.ShapeDtypeStruct((3, heads, HEAD, HALF), BF16),
        cost_estimate=pl.CostEstimate(
            flops=area * 2 * 256 * 5, bytes_accessed=heads * HALF * HEAD * 16, transcendentals=area
        ),
        name="attention_backward",
    )(*masks, stacked, stacked, stacked, mixed, logs, grads)


def picture_masks(starts):
    before = jnp.concatenate([starts[:1], starts[:-1]])
    changes = (starts != before).astype(F32)
    place = lax.iota(jnp.int32, HALF)
    number = jnp.sum(jnp.where(place[:, None] <= place[None, :], changes[:, None], 0.0), axis=0)
    row = lax.broadcasted_iota(jnp.int32, (FEATURES, HALF), 0)
    same = row.astype(F32) == number[None, :]
    listed = row < PICTURES
    mask = jnp.where(listed & ~same, MASKED_SCORE, 0.0)
    key_mask = jnp.where(listed, same.astype(F32), (row < PICTURES + 3).astype(F32))
    return mask, key_mask


LINE = 4
MESH = pl.DeviceIdType.MESH


def place_of():
    at, y = lax.axis_index("dp"), lax.axis_index("mp")
    return at // 4, (at // 2) % 2, y, at % 2


def device_of(z, x, y, core):
    return ((z * 2 + x) * 2 + core, y)


def neighbours(z, x, y, core):
    return (
        device_of(z, x, y, 1 - core), device_of(z, 1 - x, y, core), device_of(z, x, 1 - y, core)
    )


def enter(z, x, y, core, leap=None):
    barrier = pltpu.get_barrier_semaphore()
    for device in neighbours(z, x, y, core):
        pl.semaphore_signal(barrier, inc=1, device_id=device, device_id_type=MESH)

    @pl.when(z > 0)
    def _():
        pl.semaphore_signal(barrier, inc=1, device_id=device_of(z - 1, x, y, core), device_id_type=MESH)

    @pl.when(z < LINE - 1)
    def _():
        pl.semaphore_signal(barrier, inc=1, device_id=device_of(z + 1, x, y, core), device_id_type=MESH)

    if leap is not None:
        pl.semaphore_signal(barrier, inc=1, device_id=device_of(leap, x, y, core), device_id_type=MESH)
    base = 3 if leap is None else 4
    pl.semaphore_wait(barrier, base + jnp.where(z > 0, 1, 0) + jnp.where(z < LINE - 1, 1, 0))


def chunks_of(widths, pieces):
    chunks = []
    for array, (width, count) in enumerate(zip(widths, pieces)):
        tiles = -(-width // 128)
        edges = [min(width, tiles * i // count * 128) for i in range(count + 1)]
        for begin, end in zip(edges[:-1], edges[1:]):
            chunks.append((array, begin, end - begin, len(chunks) % 2 == 0))
    return chunks


def run_stages(stages, count):
    for step in range(len(stages) + count - 1):
        for chunk in range(count):
            if 0 <= step - chunk < len(stages):
                stages[step - chunk](chunk)


def gather_kernel(arrays, chunks, *refs):
    shards, wholes = refs[:arrays], refs[arrays : 2 * arrays]
    own_sem, z_send, z_recv, side_send, side_recv, core_send, core_recv = refs[2 * arrays :]
    z, x, y, core = place_of()
    other, across_x, across_y = neighbours(z, x, y, core)

    def spot(a, zz, xx, yy, holder):
        array, begin, size, _ = chunks[a]
        return wholes[array].at[yy, (zz * 2 + xx) * 2 + holder, :, pl.ds(begin, size)]

    def remote(block, send, recv, device):
        return pltpu.make_async_remote_copy(block, block, send, recv, device, MESH)

    def along_z(a, zz, upward, source):
        return remote(
            spot(a, zz, x, y, core), z_send.at[a, zz, 1 if upward else 0], z_recv.at[a, zz],
            device_of(source + (1 if upward else -1), x, y, core),
        )

    def sideways(a, stage, zz, flip, landing=False):
        over_x = chunks[a][3] == (stage == 0)
        near, far = (x, y) if over_x else (y, x)
        near, far = 1 - near if landing else near, 1 - far if flip else far
        xx, yy = (near, far) if over_x else (far, near)
        slot = zz * 2 + (1 if flip else 0)
        return remote(
            spot(a, zz, xx, yy, core), side_send.at[a, stage, slot], side_recv.at[a, stage, slot],
            across_x if over_x else across_y,
        )

    def hand_over(a, zz, fx, fy, landing=False):
        xx = 1 - x if fx else x
        yy = 1 - y if fy else y
        slot = zz * 4 + (2 if fx else 0) + (1 if fy else 0)
        return remote(
            spot(a, zz, xx, yy, 1 - core if landing else core),
            core_send.at[a, slot], core_recv.at[a, slot], other,
        )

    def launch_line_block(a, zz):
        sideways(a, 0, zz, False).start()
        sideways(a, 1, zz, False).start()
        hand_over(a, zz, False, False).start()

    def stage_begin(a):
        array, begin, size, _ = chunks[a]
        own = pltpu.make_async_copy(
            shards[array].at[:, pl.ds(begin, size)], spot(a, z, x, y, core), own_sem.at[a]
        )
        own.start()
        own.wait()

        @pl.when(z < LINE - 1)
        def _():
            along_z(a, z, True, z).start()

        @pl.when(z > 0)
        def _():
            along_z(a, z, False, z).start()

        launch_line_block(a, z)

    def stage_hop(a, hop):
        @pl.when(z >= hop)
        def _():
            along_z(a, z - hop, True, z - 1).wait_recv()

            @pl.when(z < LINE - 1)
            def _():
                along_z(a, z - hop, True, z).start()

            launch_line_block(a, z - hop)

        @pl.when(z < LINE - hop)
        def _():
            along_z(a, z + hop, False, z + 1).wait_recv()

            @pl.when(z > 0)
            def _():
                along_z(a, z + hop, False, z).start()

            launch_line_block(a, z + hop)

    def stage_turn(a):
        over_x = chunks[a][3]
        for zz in range(LINE):
            sideways(a, 0, zz, False, landing=True).wait_recv()
            sideways(a, 1, zz, True).start()
            hand_over(a, zz, over_x, not over_x).start()

    def stage_last(a):
        over_x = chunks[a][3]
        for zz in range(LINE):
            sideways(a, 1, zz, False, landing=True).wait_recv()
            hand_over(a, zz, not over_x, over_x).start()
            sideways(a, 1, zz, True, landing=True).wait_recv()
            hand_over(a, zz, True, True).start()

    def stage_close(a):
        for zz in range(LINE):
            for fx in (False, True):
                for fy in (False, True):
                    hand_over(a, zz, fx, fy, landing=True).wait_recv()
                    hand_over(a, zz, fx, fy).wait_send()
            sideways(a, 0, zz, False).wait_send()
            sideways(a, 1, zz, False).wait_send()
            sideways(a, 1, zz, True).wait_send()

            @pl.when(jnp.logical_and(z >= zz, z < LINE - 1))
            def _():
                along_z(a, zz, True, z).wait_send()

            @pl.when(jnp.logical_and(z <= zz, z > 0))
            def _():
                along_z(a, zz, False, z).wait_send()

    enter(z, x, y, core)
    hops = [partial(stage_hop, hop=hop) for hop in range(1, LINE)]
    run_stages([stage_begin, *hops, stage_turn, stage_last, stage_close], len(chunks))


def gather_blocks(shards, pieces, mp):
    rows, dp = shards[0].shape[0], 16
    chunks = chunks_of([item.shape[1] for item in shards], pieces)
    count = len(chunks)
    anywhere = pl.BlockSpec(memory_space=pl.ANY)
    dma = pltpu.SemaphoreType.DMA
    sent = sum(item.size * 2 for item in shards) * 15
    wholes = pl.pallas_call(
        partial(gather_kernel, len(shards), chunks),
        in_specs=[anywhere] * len(shards),
        out_specs=[anywhere] * len(shards),
        out_shape=[jax.ShapeDtypeStruct((mp, dp, rows, item.shape[1]), BF16) for item in shards],
        scratch_shapes=[
            dma((count,)), dma((count, LINE, 2)), dma((count, LINE)), dma((count, 2, 8)),
            dma((count, 2, 8)), dma((count, 16)), dma((count, 16)),
        ],
        compiler_params=pltpu.CompilerParams(collective_id=0, has_side_effects=True),
        cost_estimate=pl.CostEstimate(flops=0, bytes_accessed=sent, transcendentals=0),
        name="gather_blocks",
    )(*shards)
    return [whole.reshape(mp, dp * rows, whole.shape[-1]) for whole in wholes]


def scatter_kernel(arrays, chunks, *refs):
    grads, vector = refs[:arrays], refs[arrays]
    outs, vector_out = refs[arrays + 1 : 2 * arrays + 1], refs[2 * arrays + 1]
    count = len(chunks)
    rest = refs[2 * arrays + 2 :]
    held, first, second, third, up, down = (rest[i * count : (i + 1) * count] for i in range(6))
    passed = rest[6 * count]
    (
        load_sem, core_send, core_recv, one_send, one_recv, two_send, two_recv, up_send, up_recv,
        down_send, down_recv, vec_send, vec_recv,
    ) = rest[6 * count + 1 :]
    z, x, y, core = place_of()
    other, across_x, across_y = neighbours(z, x, y, core)
    leap = jnp.where(z < 2, z + 2, z - 2)
    pair = z + 1 - 2 * (z % 2)
    remote = lambda src, dst, send, recv, device: pltpu.make_async_remote_copy(
        src, dst, send, recv, device, MESH
    )

    def quarter(a, flip_near, flip_far):
        over_x = chunks[a][3]
        fx, fy = (flip_near, flip_far) if over_x else (flip_far, flip_near)
        return (1 - x if fx else x), (1 - y if fy else y)

    quarters = ((True, True), (True, False), (False, True), (False, False))

    def source(a, xx, yy, holder):
        array, begin, size, _ = chunks[a]
        return grads[array].at[yy, :, xx, holder, :, pl.ds(begin, size)]

    def load(a, i):
        xx, yy = quarter(a, *quarters[i])
        return pltpu.make_async_copy(source(a, xx, yy, core), held[a].at[i], load_sem.at[a, i])

    def share(a, i):
        xx, yy = quarter(a, *quarters[i])
        return remote(
            source(a, xx, yy, 1 - core), first[a].at[i], core_send.at[a, i], core_recv.at[a, i], other
        )

    def near(a):
        return across_x if chunks[a][3] else across_y

    def far(a):
        return across_y if chunks[a][3] else across_x

    def cross_one(a, i):
        return remote(
            held[a].at[i], second[a].at[i], one_send.at[a, i], one_recv.at[a, i], near(a)
        )

    def cross_two(a):
        return remote(held[a].at[2], third[a], two_send.at[a], two_recv.at[a], far(a))

    def add_rows(target, slot, term):
        def one(zz, unused):
            target[slot, zz] = (target[slot, zz].astype(F32) + term[zz].astype(F32)).astype(BF16)
            return unused

        lax.fori_loop(0, LINE, one, 0)

    def add_block(a, d, term):
        held[a][3, d] = (held[a][3, d].astype(F32) + term[d].astype(F32)).astype(BF16)

    def lift(a, d):
        return remote(
            held[a].at[3, d], up[a].at[d], up_send.at[a, d], up_recv.at[a, d],
            device_of(z + 1, x, y, core),
        )

    def drop(a, d):
        return remote(
            held[a].at[3, d], down[a].at[d], down_send.at[a, d], down_recv.at[a, d],
            device_of(z - 1, x, y, core),
        )

    def stage_begin(a):
        for i in range(4):
            share(a, i).start()
            load(a, i).start()

    def stage_share(a):
        for i in range(4):
            load(a, i).wait()
            share(a, i).wait_recv()
            add_rows(held[a], i, first[a].at[i])
            if i < 2:
                cross_one(a, i).start()

    def stage_one(a):
        cross_one(a, 0).wait_recv()
        add_rows(held[a], 2, second[a].at[0])
        cross_two(a).start()
        cross_one(a, 1).wait_recv()
        add_rows(held[a], 3, second[a].at[1])

    def stage_two(a):
        cross_two(a).wait_recv()
        add_rows(held[a], 3, third[a])

    def stage_line(a, hop):
        for way in (True, False):
            position = hop if way else LINE - 1 - hop
            beyond = range(LINE - 1, position, -1) if way else range(position)

            @pl.when(z == position)
            def _():
                for d in beyond:
                    if hop > 0:
                        (lift if way else drop)(a, d).wait_recv()
                        add_block(a, d, (up if way else down)[a])
                    (lift if way else drop)(a, d).start()

    def stage_finish(a):
        array, begin, size, _ = chunks[a]
        for d in range(LINE):

            @pl.when(z == d)
            def _():
                own = held[a][3, d].astype(F32)
                if d > 0:
                    lift(a, d).wait_recv()
                    own = own + up[a][d].astype(F32)
                if d < LINE - 1:
                    drop(a, d).wait_recv()
                    own = own + down[a][d].astype(F32)
                outs[array][:, begin : begin + size] = own

    def stage_close(a):
        for i in range(4):
            share(a, i).wait_send()
        cross_one(a, 0).wait_send()
        cross_one(a, 1).wait_send()
        cross_two(a).wait_send()
        for d in range(LINE):

            @pl.when(z < d)
            def _():
                lift(a, d).wait_send()

            @pl.when(z > d)
            def _():
                drop(a, d).wait_send()

    hops = (other, across_x, across_y, device_of(pair, x, y, core), device_of(leap, x, y, core))

    def exchange(k):
        return remote(passed.at[k], passed.at[k + 5], vec_send.at[k], vec_recv.at[k], hops[k])

    def vector_step(step):
        if step == 0:
            passed[0] = vector[...]
            exchange(0).start()
        elif step <= 5:
            k = step - 1
            exchange(k).wait()
            summed = passed[k] + passed[k + 5]
            if step < 5:
                passed[k + 1] = summed
                exchange(k + 1).start()
            else:
                vector_out[...] = summed

    enter(z, x, y, core, leap)
    line = [partial(stage_line, hop=hop) for hop in range(LINE - 1)]
    stages = [stage_begin, stage_share, stage_one, stage_two, *line, stage_finish, stage_close]
    for step in range(len(stages) + count - 1):
        vector_step(step)
        for chunk in range(count):
            if 0 <= step - chunk < len(stages):
                stages[step - chunk](chunk)


def scatter_blocks(parts, pieces, vector, mp):
    dp = 16
    columns = [part.shape[-1] for part in parts]
    rows = parts[0].shape[1] // dp
    chunks = chunks_of(columns, pieces)
    count = len(chunks)
    sizes = [chunk[2] for chunk in chunks]
    dma = pltpu.SemaphoreType.DMA
    vmem = pl.BlockSpec(memory_space=pltpu.VMEM)
    lines = -(-vector.shape[0] // 1024) * 8
    padded = jnp.pad(vector, (0, lines * 128 - vector.shape[0])).reshape(lines, 128)
    blocks = lambda *lead: [pltpu.VMEM((*lead, LINE, rows, size), BF16) for size in sizes]
    sent = sum(columns) * rows * 2 * 30
    *outs, summed = pl.pallas_call(
        partial(scatter_kernel, len(parts), chunks),
        in_specs=[pl.BlockSpec(memory_space=pl.ANY)] * len(parts) + [vmem],
        out_specs=[vmem] * (len(parts) + 1),
        out_shape=[jax.ShapeDtypeStruct((rows, width), F32) for width in columns]
        + [jax.ShapeDtypeStruct((lines, 128), F32)],
        scratch_shapes=[
            *blocks(4), *blocks(4), *blocks(2), *blocks(), *blocks(), *blocks(),
            pltpu.VMEM((10, lines, 128), F32),
            dma((count, 4)), dma((count, 4)), dma((count, 4)), dma((count, 2)), dma((count, 2)),
            dma((count,)), dma((count,)), dma((count, LINE)), dma((count, LINE)), dma((count, LINE)),
            dma((count, LINE)), dma((5,)), dma((5,)),
        ],
        compiler_params=pltpu.CompilerParams(collective_id=1, has_side_effects=True),
        cost_estimate=pl.CostEstimate(flops=0, bytes_accessed=sent, transcendentals=0),
        name="scatter_blocks",
    )(*[part.reshape(mp, LINE, 2, 2, rows, part.shape[-1]) for part in parts], padded)
    return outs, summed.reshape(-1)[: vector.shape[0]]


def gradient_kernel(count, left_ref, *refs):
    rights, out_ref = refs[:count], refs[count]
    columns = rights[0].shape[0]
    for j in range(count):

        @pl.when(pl.program_id(0) == j)
        def _():
            out_ref[0, :, :columns] = dot(left_ref[...], rights[j][...], 1, 1).astype(BF16)

    if columns < out_ref.shape[2]:
        extra = out_ref.shape[2] - columns
        out_ref[0, :, columns:] = jnp.zeros((out_ref.shape[1], extra), BF16)


def weight_gradient(left, rights, lanes):
    width, tokens = left.shape
    count, columns = len(rights), rights[0].shape[0]
    padded = columns + -columns % lanes
    tile = 384
    whole = lambda j, m: (0, 0)
    return pl.pallas_call(
        partial(gradient_kernel, count),
        grid=(count, width // tile),
        in_specs=[pl.BlockSpec((tile, tokens), lambda j, m: (m, 0))]
        + [pl.BlockSpec((columns, tokens), whole)] * count,
        out_specs=pl.BlockSpec((1, tile, padded), lambda j, m: (j, m, 0)),
        out_shape=jax.ShapeDtypeStruct((count, width, padded), BF16),
        cost_estimate=pl.CostEstimate(
            flops=2 * width * tokens * columns * count,
            bytes_accessed=2 * count * (width * padded + columns * tokens) + 2 * width * tokens,
            transcendentals=0,
        ),
        name="weight_gradient",
    )(left, *rights)


def local_norm(values):
    centre = jnp.mean(values, axis=1, keepdims=True)
    centred = values - centre
    rstd = lax.rsqrt(jnp.mean(centred * centred, axis=1, keepdims=True) + EPSILON)
    return centred * rstd, rstd


def norm_backward(grad_normed, normed, rstd, gain):
    scaled = grad_normed * gain
    mean_grad = jnp.mean(scaled, axis=1, keepdims=True)
    mean_cross = jnp.mean(scaled * normed, axis=1, keepdims=True)
    return rstd * (scaled - mean_grad - normed * mean_cross)


def gelu_parts(rows):
    cubic = math.sqrt(2.0 / math.pi) * (rows + 0.044715 * rows * rows * rows)
    bend = jnp.tanh(cubic)
    value = 0.5 * rows * (1.0 + bend)
    slope = 0.5 * (1.0 + bend) + 0.5 * rows * (1.0 - bend * bend) * (
        math.sqrt(2.0 / math.pi) * (1.0 + 3.0 * 0.044715 * rows * rows)
    )
    return value, slope


def total(parts):
    out = parts[0]
    for part in parts[1:]:
        out = out + part
    return out


def body(
    inputs,
    picture_start,
    prenorm_gain,
    prenorm_shift,
    query_weight,
    query_bias,
    key_weight,
    value_weight,
    value_bias,
    output_weight,
    output_bias,
    midnorm_gain,
    midnorm_shift,
    hidden_weight,
    hidden_bias,
    project_weight,
    project_bias,
    cotangent,
    *,
    dp,
    mp,
):
    tokens, width = inputs.shape
    shard = query_weight.shape[1]
    hidden = hidden_weight.shape[1]
    group = HALF // tokens
    me = lax.axis_index("mp")
    groups = [list(range(i, i + group)) for i in range(0, mp, group)]

    fitted = dp == 16 and mp == 2
    lanes = 256

    def gather(weight):
        whole = lax.all_gather(weight, ("mp", "dp"), axis=0, tiled=True)
        return whole.reshape(mp, width, weight.shape[1])

    def scatter(parts, columns):
        whole = parts.reshape(mp * width, parts.shape[2])
        mine = lax.psum_scatter(whole, ("mp", "dp"), scatter_dimension=0, tiled=True)
        return lax.optimization_barrier(mine)[:, :columns].astype(F32)

    def to_heads(part):
        kinds = part.shape[0]
        if group == 1:
            return part
        part = part.reshape(kinds, group, HEADS // group, HEAD, tokens).transpose(1, 0, 2, 3, 4)
        part = lax.all_to_all(part, "mp", 0, 0, axis_index_groups=groups, tiled=True)
        return part.transpose(1, 2, 3, 0, 4).reshape(kinds, HEADS // group, HEAD, HALF)

    def from_heads(part):
        kinds = part.shape[0]
        if group == 1:
            return part
        part = part.reshape(kinds, HEADS // group, HEAD, group, tokens).transpose(3, 0, 1, 2, 4)
        part = lax.all_to_all(part, "mp", 0, 0, axis_index_groups=groups, tiled=True)
        return part.transpose(1, 0, 2, 3, 4).reshape(kinds, HEADS, HEAD, tokens)

    query_bias_all, value_bias_all, hidden_bias_all = (
        lax.all_gather(item, "mp", axis=0, tiled=False)
        for item in (query_bias, value_bias, hidden_bias)
    )
    half = me // group
    starts = lax.dynamic_slice_in_dim(picture_start, half * HALF, HALF)
    masks = picture_masks(starts)

    attn_shard = jnp.concatenate([query_weight, key_weight, value_weight], axis=1)
    if fitted:
        attn_weights, output_all = gather_blocks([attn_shard, output_weight.T], (2, 2), mp)
        attn_weights, hidden_shard, project_shard = lax.optimization_barrier(
            (attn_weights, hidden_weight, project_weight)
        )
    else:
        attn_weights, output_all = gather(attn_shard), gather(output_weight.T)
        hidden_shard, project_shard = hidden_weight, project_weight
    hidden_all = gather(hidden_shard)
    project_all = gather(project_shard.T)

    residual_in = inputs.astype(F32)
    normed_pre, rstd_pre = local_norm(residual_in)
    attn_in = (normed_pre * prenorm_gain + prenorm_shift).astype(BF16)

    stacks = []
    for j in range(mp):
        bias = jnp.concatenate(
            [query_bias_all[j], jnp.zeros((shard,), F32), value_bias_all[j]], axis=0
        )
        rows = (dot(attn_weights[j], attn_in, 0, 1) + bias[:, None]).astype(BF16)
        stacks.append(rows.reshape(3, shard // HEAD, HEAD, tokens))
    if group == 1:
        pieces = stacks
    else:
        pieces = [to_heads(jnp.concatenate(stacks, axis=1))]
    mixed_pieces, log_pieces, tops = [], [], []
    for piece in pieces:
        mixed_piece, log_piece, top_piece = attention_forward(masks, piece)
        mixed_pieces.append(mixed_piece)
        log_pieces.append(log_piece)
        tops.append(jnp.max(top_piece, axis=(1, 2)))
    peak_here = jnp.concatenate(tops) / LOG2E
    if group == 1:
        mixed = [piece.reshape(shard, tokens) for piece in mixed_pieces]
    else:
        rows = from_heads(mixed_pieces[0][None])[0].reshape(mp, shard, tokens)
        mixed = [rows[j] for j in range(mp)]
        spread = jnp.full((HEADS,), MASKED_SCORE, F32)
        peak_here = lax.dynamic_update_slice_in_dim(
            spread, peak_here, (me % group) * (HEADS // group), 0
        )
    residual_mid = (
        residual_in + total([dot(mixed[j], output_all[j], 0, 1) for j in range(mp)]) + output_bias
    )
    normed_mid, rstd_mid = local_norm(residual_mid)
    mlp_in = (normed_mid * midnorm_gain + midnorm_shift).astype(BF16)
    activated, slopes = [], []
    for j in range(mp):
        value, slope = gelu_parts(dot(hidden_all[j], mlp_in, 0, 1) + hidden_bias_all[j][:, None])
        activated.append(value.astype(BF16))
        slopes.append(slope.astype(BF16))
    activated, slopes = lax.optimization_barrier((activated, slopes))
    project_parts = weight_gradient(cotangent.T, activated, lanes)
    project_parts, late_cotangent = lax.optimization_barrier((project_parts, cotangent))
    with jax.named_scope("scatter_project"):
        project_grad = scatter(project_parts, hidden)
    grad_up = [
        (dot(project_all[j], late_cotangent, 0, 1) * slopes[j].astype(F32)).astype(BF16)
        for j in range(mp)
    ]
    grad_up = lax.optimization_barrier(grad_up)
    hidden_parts = weight_gradient(mlp_in.T, grad_up, lanes)
    hidden_parts, grad_up, activated = lax.optimization_barrier((hidden_parts, grad_up, activated))
    with jax.named_scope("scatter_hidden"):
        hidden_grad = scatter(hidden_parts, hidden)
    final_rows = (
        residual_mid
        + total([dot(activated[j], project_all[j], 0, 1) for j in range(mp)])
        + project_bias
    )
    layer_output = final_rows.astype(BF16)

    grad_output = cotangent.astype(F32)
    grad_mid = total([dot(grad_up[j], hidden_all[j], 0, 1) for j in range(mp)])
    grad_resid = grad_output + norm_backward(grad_mid, normed_mid, rstd_mid, midnorm_gain)
    grad_branch = grad_resid.astype(BF16)
    output_parts = weight_gradient(grad_branch.T, mixed, 1 if fitted else lanes)
    grad_mixed = [
        dot(output_all[j], grad_branch, 0, 1).astype(BF16).reshape(shard // HEAD, HEAD, tokens)
        for j in range(mp)
    ]
    if group > 1:
        grad_mixed = [to_heads(jnp.concatenate(grad_mixed, axis=0)[None])[0]]
    grad_pieces = [
        attention_backward(masks, piece, mixed_piece, log_piece, grads)
        for piece, mixed_piece, log_piece, grads in zip(
            pieces, mixed_pieces, log_pieces, grad_mixed
        )
    ]
    if group > 1:
        whole = from_heads(grad_pieces[0]).reshape(3, mp, shard // HEAD, HEAD, tokens)
        grad_pieces = [whole[:, j] for j in range(mp)]
    grad_rows = [piece.reshape(3 * shard, tokens) for piece in grad_pieces]
    attn_parts = weight_gradient(attn_in.T, grad_rows, 1 if fitted else lanes)
    grad_pre = total([dot(grad_rows[j], attn_weights[j], 0, 1) for j in range(mp)])
    inputs_gradient = grad_resid + norm_backward(grad_pre, normed_pre, rstd_pre, prenorm_gain)

    row_sums = [jnp.sum(rows.astype(F32), axis=1) for rows in grad_rows]
    head_parts = (
        jnp.stack([sums[:shard] for sums in row_sums]),
        jnp.stack([sums[2 * shard :] for sums in row_sums]),
        jnp.stack([jnp.sum(part.astype(F32), axis=1) for part in grad_up]),
    )
    norm_parts = (
        jnp.sum(grad_pre * normed_pre, axis=0),
        jnp.sum(grad_pre, axis=0),
        jnp.sum(grad_branch.astype(F32), axis=0),
        jnp.sum(grad_mid * normed_mid, axis=0),
        jnp.sum(grad_mid, axis=0),
        jnp.sum(grad_output, axis=0),
    )
    slot = lax.axis_index("dp") * mp + me
    peak_slots = jnp.where(lax.iota(jnp.int32, dp * mp)[:, None] == slot, peak_here[None, :], 0.0)
    flat = jnp.concatenate([item.reshape(-1) for item in (*head_parts, *norm_parts, peak_slots)])
    if fitted:
        output_parts, project_grad = lax.optimization_barrier((output_parts, project_grad))
        (attn_grad, output_grad), flat = scatter_blocks([attn_parts, output_parts], (2, 2), flat, mp)
    else:
        attn_grad, output_grad = scatter(attn_parts, 3 * shard), scatter(output_parts, shard)
        flat = lax.psum(flat, ("dp", "mp"))
    ends = [mp * shard, mp * shard, mp * hidden] + [width] * 6
    sums, at = [], 0
    for size in ends:
        sums.append(flat[at : at + size])
        at += size
    peak_all = jnp.max(flat[at:].reshape(dp * mp, HEADS), axis=0)
    logit_peak = lax.dynamic_slice_in_dim(peak_all, me * (HEADS // mp), HEADS // mp)
    factor = jnp.repeat(jnp.sqrt(CLIP_LIMIT / jnp.maximum(logit_peak, CLIP_LIMIT)), HEAD)
    clipped_query = query_weight.astype(F32) * factor[None, :]
    clipped_key = key_weight.astype(F32) * factor[None, :]
    query_bias_grad, value_bias_grad, hidden_bias_grad = (
        lax.dynamic_index_in_dim(item.reshape(mp, -1), me, keepdims=False) for item in sums[:3]
    )
    return (
        layer_output,
        inputs_gradient,
        sums[3],
        sums[4],
        attn_grad[:, :shard],
        query_bias_grad,
        attn_grad[:, shard : 2 * shard],
        attn_grad[:, 2 * shard :],
        value_bias_grad,
        output_grad.T,
        sums[5],
        sums[6],
        sums[7],
        hidden_grad,
        hidden_bias_grad,
        project_grad.T,
        sums[8],
        logit_peak,
        clipped_query,
        clipped_key,
    )


def solution(mesh):
    rows = P(("dp", "mp"), None)
    split = P("dp", "mp")
    turned = P("mp", "dp")
    heads = P("mp")
    whole = P()
    placed = (
        rows, P("dp"), whole, whole, split, heads, split, split, heads, turned, whole, whole, whole,
        split, heads, turned, whole, rows,
    )
    given = (
        rows, rows, whole, whole, split, heads, split, split, heads, turned, whole, whole, whole,
        split, heads, turned, whole, heads, split, split,
    )
    return jax.shard_map(
        partial(body, dp=mesh.shape["dp"], mp=mesh.shape["mp"]),
        mesh=mesh,
        in_specs=placed,
        out_specs=given,
        check_vma=False,
    )
```

```python
import math
from functools import partial

import jax
import jax.numpy as jnp
from jax import lax
from jax.experimental import pallas as pl
from jax.experimental.pallas import tpu as pltpu
from jax.sharding import PartitionSpec as P

HEAD = 72
HEADS = 16
ROW = 2048
HALF = 1024
EPSILON = 1e-06
CLIP_LIMIT = 7.0
MASKED_SCORE = -1e30
FEATURES = 16
PICTURES = 10
QUERY_BLOCK = 256
FORWARD_BLOCK = 512
SCALE = HEAD ** (-0.5)
LOG2E = 1.0 / math.log(2.0)
EXPONENT = SCALE * LOG2E
F32 = jnp.float32
BF16 = jnp.bfloat16


def dot(left, right, left_dim=1, right_dim=0):
    return lax.dot_general(
        left, right, (((left_dim,), (right_dim,)), ((), ())), preferred_element_type=F32
    )


def split_terms(value, count):
    terms = []
    for _ in range(count):
        term = value.astype(BF16).astype(F32)
        terms.append(term)
        value = value - term
    return terms


def query_operand(query, features):
    pad = jnp.zeros((8, query.shape[1]), F32)
    high, low = split_terms(query.astype(F32) * EXPONENT, 2)
    return jnp.concatenate([high, pad, low, pad, features], axis=0).astype(BF16)


def key_operand(key, features):
    pad = jnp.zeros((8, key.shape[1]), F32)
    wide = key.astype(F32)
    stacked = jnp.concatenate([wide, pad, wide, pad, features], axis=0)
    return stacked.T.astype(BF16)


def rows_below(wide, extra):
    width = wide.shape[1]
    row = lax.broadcasted_iota(jnp.int32, (8, width), 0)
    block = jnp.zeros((8, width), F32)
    for position, line in enumerate(extra):
        block = jnp.where(row == position, line, block)
    return jnp.concatenate([wide, block], axis=0)


def forward_kernel(mask_ref, key_mask_ref, query_ref, key_ref, value_ref, mixed_ref, log_ref, top_ref):
    query_rows = query_operand(query_ref[0, 0], mask_ref[...])
    key_rows = key_operand(key_ref[0, 0], key_mask_ref[...])
    value_rows = rows_below(value_ref[0, 0].astype(F32), [jnp.ones((1, 1), F32)]).astype(BF16)
    blocks = [slice(begin, begin + FORWARD_BLOCK) for begin in range(0, HALF, FORWARD_BLOCK)]
    following = dot(key_rows, query_rows[:, blocks[0]])
    for number, block in enumerate(blocks):
        scores = following
        if number + 1 < len(blocks):
            following = dot(key_rows, query_rows[:, blocks[number + 1]])
        top = jnp.max(scores, axis=0, keepdims=True)
        weights = jnp.exp2(scores - top).astype(BF16)
        summed = dot(value_rows, weights)
        total = summed[HEAD : HEAD + 1]
        mixed_ref[0, :, block] = (summed[:HEAD] / total).astype(BF16)
        log_ref[0, :, block] = top + jnp.log2(total)
        top_ref[0, :, block] = top


def backward_kernel(
    mask_ref, key_mask_ref, query_ref, key_ref, value_ref, mixed_ref, log_ref, grad_ref, out_ref
):
    query, key = query_ref[0, 0], key_ref[0, 0]
    grad = grad_ref[0]
    row = lax.broadcasted_iota(jnp.int32, (FEATURES, HALF), 0)
    features = mask_ref[...]
    for position, term in enumerate(split_terms(-log_ref[0], 3)):
        features = jnp.where(row == PICTURES + position, term, features)
    query_rows = query_operand(query, features)
    key_rows = key_operand(key, key_mask_ref[...])
    grad_wide = grad.astype(F32)
    delta = jnp.sum(grad_wide * mixed_ref[0].astype(F32), axis=0, keepdims=True)
    grad_rows = rows_below(grad_wide, split_terms(-delta, 2)).astype(BF16)
    one = jnp.ones((1, 1), F32)
    value_rows = rows_below(value_ref[0, 0].astype(F32), [one, one]).T.astype(BF16)
    query_cols = query.astype(F32).T.astype(BF16)
    grad_cols = grad_wide.T.astype(BF16)
    grad_key = jnp.zeros((HALF, HEAD), F32)
    grad_value = jnp.zeros((HALF, HEAD), F32)
    for begin in range(0, HALF, QUERY_BLOCK):
        block = slice(begin, begin + QUERY_BLOCK)
        weights = jnp.exp2(dot(key_rows, query_rows[:, block]))
        slopes = dot(value_rows, grad_rows[:, block])
        grad_scores = (weights * slopes).astype(BF16)
        grad_value = grad_value + dot(weights.astype(BF16), grad_cols[block])
        grad_key = grad_key + dot(grad_scores, query_cols[block])
        out_ref[0, 0, :, block] = (dot(key, grad_scores) * SCALE).astype(BF16)
    out_ref[1, 0] = (grad_key * SCALE).T.astype(BF16)
    out_ref[2, 0] = grad_value.T.astype(BF16)


def head_specs():
    features = pl.BlockSpec((FEATURES, HALF), lambda h: (0, 0))
    part = [pl.BlockSpec((1, 1, HEAD, HALF), lambda h, i=i: (i, h, 0, 0)) for i in range(3)]
    head = pl.BlockSpec((1, HEAD, HALF), lambda h: (h, 0, 0))
    line = pl.BlockSpec((1, 1, HALF), lambda h: (h, 0, 0))
    return features, part, head, line


def attention_forward(masks, stacked):
    heads = stacked.shape[1]
    features, part, head, line = head_specs()
    area = heads * HALF * HALF
    return pl.pallas_call(
        forward_kernel,
        grid=(heads,),
        in_specs=[features, features, *part],
        out_specs=(head, line, line),
        out_shape=(
            jax.ShapeDtypeStruct((heads, HEAD, HALF), BF16),
            jax.ShapeDtypeStruct((heads, 1, HALF), F32),
            jax.ShapeDtypeStruct((heads, 1, HALF), F32),
        ),
        cost_estimate=pl.CostEstimate(
            flops=area * 2 * 256 * 2, bytes_accessed=heads * HALF * HEAD * 8, transcendentals=area
        ),
        name="attention_forward",
    )(*masks, stacked, stacked, stacked)


def attention_backward(masks, stacked, mixed, logs, grads):
    heads = stacked.shape[1]
    features, part, head, line = head_specs()
    area = heads * HALF * HALF
    return pl.pallas_call(
        backward_kernel,
        grid=(heads,),
        in_specs=[features, features, *part, head, line, head],
        out_specs=pl.BlockSpec((3, 1, HEAD, HALF), lambda h: (0, h, 0, 0)),
        out_shape=jax.ShapeDtypeStruct((3, heads, HEAD, HALF), BF16),
        cost_estimate=pl.CostEstimate(
            flops=area * 2 * 256 * 5, bytes_accessed=heads * HALF * HEAD * 16, transcendentals=area
        ),
        name="attention_backward",
    )(*masks, stacked, stacked, stacked, mixed, logs, grads)


def picture_masks(starts):
    before = jnp.concatenate([starts[:1], starts[:-1]])
    changes = (starts != before).astype(F32)
    place = lax.iota(jnp.int32, HALF)
    number = jnp.sum(jnp.where(place[:, None] <= place[None, :], changes[:, None], 0.0), axis=0)
    row = lax.broadcasted_iota(jnp.int32, (FEATURES, HALF), 0)
    same = row.astype(F32) == number[None, :]
    listed = row < PICTURES
    mask = jnp.where(listed & ~same, MASKED_SCORE, 0.0)
    key_mask = jnp.where(listed, same.astype(F32), (row < PICTURES + 3).astype(F32))
    return mask, key_mask


LINE = 4
LEVEL_G = 6
LEVEL_S = 2
MESH = pl.DeviceIdType.MESH


def place_of():
    at, y = lax.axis_index("dp"), lax.axis_index("mp")
    return at // 4, (at // 2) % 2, y, at % 2


def device_of(z, x, y, core):
    return ((z * 2 + x) * 2 + core, y)


def neighbours(z, x, y, core):
    return (
        device_of(z, x, y, 1 - core), device_of(z, 1 - x, y, core), device_of(z, x, 1 - y, core)
    )


def enter(z, x, y, core, leap=None):
    barrier = pltpu.get_barrier_semaphore()
    for device in neighbours(z, x, y, core):
        pl.semaphore_signal(barrier, inc=1, device_id=device, device_id_type=MESH)

    @pl.when(z > 0)
    def _():
        pl.semaphore_signal(barrier, inc=1, device_id=device_of(z - 1, x, y, core), device_id_type=MESH)

    @pl.when(z < LINE - 1)
    def _():
        pl.semaphore_signal(barrier, inc=1, device_id=device_of(z + 1, x, y, core), device_id_type=MESH)

    if leap is not None:
        pl.semaphore_signal(barrier, inc=1, device_id=device_of(leap, x, y, core), device_id_type=MESH)
    base = 3 if leap is None else 4
    pl.semaphore_wait(barrier, base + jnp.where(z > 0, 1, 0) + jnp.where(z < LINE - 1, 1, 0))


def chunks_of(widths, pieces):
    chunks = []
    for array, (width, count) in enumerate(zip(widths, pieces)):
        tiles = -(-width // 128)
        edges = [min(width, tiles * i // count * 128) for i in range(count + 1)]
        for begin, end in zip(edges[:-1], edges[1:]):
            chunks.append((array, begin, end - begin, len(chunks) % 2 == 0))
    return chunks


def run_stages(stages, count, level, between=lambda step: None):
    for stage in stages[:level]:
        for chunk in range(count):
            stage(chunk)
    rest = stages[level:]
    for step in range(len(rest) + count - 1):
        between(step)
        for chunk in range(count):
            if 0 <= step - chunk < len(rest):
                rest[step - chunk](chunk)


def gather_kernel(arrays, chunks, *refs):
    shards, lines = refs[:arrays], refs[arrays]
    wholes, both = refs[arrays + 1 : 2 * arrays + 1], refs[2 * arrays + 1]
    (
        own_sem, z_send, z_recv, side_send, side_recv, core_send, core_recv, line_own, line_send,
        line_recv,
    ) = refs[2 * arrays + 2 :]
    z, x, y, core = place_of()
    other, across_x, across_y = neighbours(z, x, y, core)

    def spot(a, zz, xx, yy, holder):
        array, begin, size, _ = chunks[a]
        return wholes[array].at[yy, (zz * 2 + xx) * 2 + holder, :, pl.ds(begin, size)]

    def remote(block, send, recv, device):
        return pltpu.make_async_remote_copy(block, block, send, recv, device, MESH)

    def along_z(a, zz, upward, source):
        return remote(
            spot(a, zz, x, y, core), z_send.at[a, zz, 1 if upward else 0], z_recv.at[a, zz],
            device_of(source + (1 if upward else -1), x, y, core),
        )

    def sideways(a, stage, zz, flip, landing=False):
        over_x = chunks[a][3] == (stage == 0)
        near, far = (x, y) if over_x else (y, x)
        near, far = 1 - near if landing else near, 1 - far if flip else far
        xx, yy = (near, far) if over_x else (far, near)
        slot = zz * 2 + (1 if flip else 0)
        return remote(
            spot(a, zz, xx, yy, core), side_send.at[a, stage, slot], side_recv.at[a, stage, slot],
            across_x if over_x else across_y,
        )

    def hand_over(a, zz, fx, fy, landing=False):
        xx = 1 - x if fx else x
        yy = 1 - y if fy else y
        slot = zz * 4 + (2 if fx else 0) + (1 if fy else 0)
        return remote(
            spot(a, zz, xx, yy, 1 - core if landing else core),
            core_send.at[a, slot], core_recv.at[a, slot], other,
        )

    def launch_line_block(a, zz):
        sideways(a, 0, zz, False).start()
        sideways(a, 1, zz, False).start()
        hand_over(a, zz, False, False).start()

    def stage_begin(a):
        array, begin, size, _ = chunks[a]
        own = pltpu.make_async_copy(
            shards[array].at[:, pl.ds(begin, size)], spot(a, z, x, y, core), own_sem.at[a]
        )
        own.start()
        own.wait()

        @pl.when(z < LINE - 1)
        def _():
            along_z(a, z, True, z).start()

        @pl.when(z > 0)
        def _():
            along_z(a, z, False, z).start()

        launch_line_block(a, z)

    def stage_hop(a, hop):
        @pl.when(z >= hop)
        def _():
            along_z(a, z - hop, True, z - 1).wait_recv()

            @pl.when(z < LINE - 1)
            def _():
                along_z(a, z - hop, True, z).start()

            launch_line_block(a, z - hop)

        @pl.when(z < LINE - hop)
        def _():
            along_z(a, z + hop, False, z + 1).wait_recv()

            @pl.when(z > 0)
            def _():
                along_z(a, z + hop, False, z).start()

            launch_line_block(a, z + hop)

    def stage_turn(a):
        over_x = chunks[a][3]
        for zz in range(LINE):
            sideways(a, 0, zz, False, landing=True).wait_recv()
            sideways(a, 1, zz, True).start()
            hand_over(a, zz, over_x, not over_x).start()

    def stage_last(a):
        over_x = chunks[a][3]
        for zz in range(LINE):
            sideways(a, 1, zz, False, landing=True).wait_recv()
            hand_over(a, zz, not over_x, over_x).start()
            sideways(a, 1, zz, True, landing=True).wait_recv()
            hand_over(a, zz, True, True).start()

    def stage_close(a):
        for zz in range(LINE):
            for fx in (False, True):
                for fy in (False, True):
                    hand_over(a, zz, fx, fy, landing=True).wait_recv()
                    hand_over(a, zz, fx, fy).wait_send()
            sideways(a, 0, zz, False).wait_send()
            sideways(a, 1, zz, False).wait_send()
            sideways(a, 1, zz, True).wait_send()

            @pl.when(jnp.logical_and(z >= zz, z < LINE - 1))
            def _():
                along_z(a, zz, True, z).wait_send()

            @pl.when(jnp.logical_and(z <= zz, z > 0))
            def _():
                along_z(a, zz, False, z).wait_send()

    enter(z, x, y, core)
    own_lines = pltpu.make_async_copy(lines, both.at[y], line_own)
    sent_lines = pltpu.make_async_remote_copy(
        lines, both.at[y], line_send, line_recv, across_y, MESH
    )
    landed_lines = pltpu.make_async_remote_copy(
        lines, both.at[1 - y], line_send, line_recv, across_y, MESH
    )
    own_lines.start()
    sent_lines.start()
    hops = [partial(stage_hop, hop=hop) for hop in range(1, LINE)]
    run_stages([stage_begin, *hops, stage_turn, stage_last, stage_close], len(chunks), LEVEL_G)
    own_lines.wait()
    sent_lines.wait_send()
    landed_lines.wait_recv()


def gather_blocks(shards, pieces, lines, mp):
    rows, dp = shards[0].shape[0], 16
    chunks = chunks_of([item.shape[1] for item in shards], pieces)
    count = len(chunks)
    anywhere = pl.BlockSpec(memory_space=pl.ANY)
    dma = pltpu.SemaphoreType.DMA
    sent = sum(item.size * 2 for item in shards) * 15
    *wholes, both = pl.pallas_call(
        partial(gather_kernel, len(shards), chunks),
        in_specs=[anywhere] * (len(shards) + 1),
        out_specs=[anywhere] * (len(shards) + 1),
        out_shape=[jax.ShapeDtypeStruct((mp, dp, rows, item.shape[1]), BF16) for item in shards]
        + [jax.ShapeDtypeStruct((mp, *lines.shape), F32)],
        scratch_shapes=[
            dma((count,)), dma((count, LINE, 2)), dma((count, LINE)), dma((count, 2, 8)),
            dma((count, 2, 8)), dma((count, 16)), dma((count, 16)), dma(()), dma(()), dma(()),
        ],
        compiler_params=pltpu.CompilerParams(collective_id=0, has_side_effects=True),
        cost_estimate=pl.CostEstimate(flops=0, bytes_accessed=sent, transcendentals=0),
        name="gather_blocks",
    )(*shards, lines)
    return [whole.reshape(mp, dp * rows, whole.shape[-1]) for whole in wholes], both


def scatter_kernel(arrays, chunks, *refs):
    grads, vector = refs[:arrays], refs[arrays]
    outs, vector_out = refs[arrays + 1 : 2 * arrays + 1], refs[2 * arrays + 1]
    count = len(chunks)
    rest = refs[2 * arrays + 2 :]
    held, first, second, third, up, down = (rest[i * count : (i + 1) * count] for i in range(6))
    passed = rest[6 * count]
    (
        load_sem, core_send, core_recv, one_send, one_recv, two_send, two_recv, up_send, up_recv,
        down_send, down_recv, vec_send, vec_recv,
    ) = rest[6 * count + 1 :]
    z, x, y, core = place_of()
    other, across_x, across_y = neighbours(z, x, y, core)
    leap = jnp.where(z < 2, z + 2, z - 2)
    pair = z + 1 - 2 * (z % 2)
    remote = lambda src, dst, send, recv, device: pltpu.make_async_remote_copy(
        src, dst, send, recv, device, MESH
    )

    def quarter(a, flip_near, flip_far):
        over_x = chunks[a][3]
        fx, fy = (flip_near, flip_far) if over_x else (flip_far, flip_near)
        return (1 - x if fx else x), (1 - y if fy else y)

    quarters = ((True, True), (True, False), (False, True), (False, False))

    def source(a, xx, yy, holder):
        array, begin, size, _ = chunks[a]
        return grads[array].at[yy, :, xx, holder, :, pl.ds(begin, size)]

    def load(a, i):
        xx, yy = quarter(a, *quarters[i])
        return pltpu.make_async_copy(source(a, xx, yy, core), held[a].at[i], load_sem.at[a, i])

    def share(a, i):
        xx, yy = quarter(a, *quarters[i])
        return remote(
            source(a, xx, yy, 1 - core), first[a].at[i], core_send.at[a, i], core_recv.at[a, i], other
        )

    def near(a):
        return across_x if chunks[a][3] else across_y

    def far(a):
        return across_y if chunks[a][3] else across_x

    def cross_one(a, i):
        return remote(
            held[a].at[i], second[a].at[i], one_send.at[a, i], one_recv.at[a, i], near(a)
        )

    def cross_two(a):
        return remote(held[a].at[2], third[a], two_send.at[a], two_recv.at[a], far(a))

    def add_rows(target, slot, term):
        def one(zz, unused):
            target[slot, zz] = (target[slot, zz].astype(F32) + term[zz].astype(F32)).astype(BF16)
            return unused

        lax.fori_loop(0, LINE, one, 0)

    def add_block(a, d, term):
        held[a][3, d] = (held[a][3, d].astype(F32) + term[d].astype(F32)).astype(BF16)

    def lift(a, d):
        return remote(
            held[a].at[3, d], up[a].at[d], up_send.at[a, d], up_recv.at[a, d],
            device_of(z + 1, x, y, core),
        )

    def drop(a, d):
        return remote(
            held[a].at[3, d], down[a].at[d], down_send.at[a, d], down_recv.at[a, d],
            device_of(z - 1, x, y, core),
        )

    def stage_begin(a):
        for i in range(4):
            share(a, i).start()
            load(a, i).start()

    def stage_share(a):
        for i in range(4):
            load(a, i).wait()
            share(a, i).wait_recv()
            add_rows(held[a], i, first[a].at[i])
            if i < 2:
                cross_one(a, i).start()

    def stage_one(a):
        cross_one(a, 0).wait_recv()
        add_rows(held[a], 2, second[a].at[0])
        cross_two(a).start()
        cross_one(a, 1).wait_recv()
        add_rows(held[a], 3, second[a].at[1])

    def stage_two(a):
        cross_two(a).wait_recv()
        add_rows(held[a], 3, third[a])

    def stage_line(a, hop):
        for way in (True, False):
            position = hop if way else LINE - 1 - hop
            beyond = range(LINE - 1, position, -1) if way else range(position)

            @pl.when(z == position)
            def _():
                for d in beyond:
                    if hop > 0:
                        (lift if way else drop)(a, d).wait_recv()
                        add_block(a, d, (up if way else down)[a])
                    (lift if way else drop)(a, d).start()

    def stage_finish(a):
        array, begin, size, _ = chunks[a]
        for d in range(LINE):

            @pl.when(z == d)
            def _():
                own = held[a][3, d].astype(F32)
                if d > 0:
                    lift(a, d).wait_recv()
                    own = own + up[a][d].astype(F32)
                if d < LINE - 1:
                    drop(a, d).wait_recv()
                    own = own + down[a][d].astype(F32)
                outs[array][:, begin : begin + size] = own

    def stage_close(a):
        for i in range(4):
            share(a, i).wait_send()
        cross_one(a, 0).wait_send()
        cross_one(a, 1).wait_send()
        cross_two(a).wait_send()
        for d in range(LINE):

            @pl.when(z < d)
            def _():
                lift(a, d).wait_send()

            @pl.when(z > d)
            def _():
                drop(a, d).wait_send()

    hops = (other, across_x, across_y, device_of(pair, x, y, core), device_of(leap, x, y, core))

    def exchange(k):
        return remote(passed.at[k], passed.at[k + 5], vec_send.at[k], vec_recv.at[k], hops[k])

    def vector_step(step):
        if step == 0:
            passed[0] = vector[...]
            exchange(0).start()
        elif step <= 5:
            k = step - 1
            exchange(k).wait()
            summed = passed[k] + passed[k + 5]
            if step < 5:
                passed[k + 1] = summed
                exchange(k + 1).start()
            else:
                vector_out[...] = summed

    enter(z, x, y, core, leap)
    line = [partial(stage_line, hop=hop) for hop in range(LINE - 1)]
    stages = [stage_begin, stage_share, stage_one, stage_two, *line, stage_finish, stage_close]
    run_stages(stages, count, LEVEL_S, vector_step)


def scatter_blocks(parts, pieces, vector, mp):
    dp = 16
    columns = [part.shape[-1] for part in parts]
    rows = parts[0].shape[1] // dp
    chunks = chunks_of(columns, pieces)
    count = len(chunks)
    sizes = [chunk[2] for chunk in chunks]
    dma = pltpu.SemaphoreType.DMA
    vmem = pl.BlockSpec(memory_space=pltpu.VMEM)
    lines = -(-vector.shape[0] // 1024) * 8
    padded = jnp.pad(vector, (0, lines * 128 - vector.shape[0])).reshape(lines, 128)
    blocks = lambda *lead: [pltpu.VMEM((*lead, LINE, rows, size), BF16) for size in sizes]
    sent = sum(columns) * rows * 2 * 30
    *outs, summed = pl.pallas_call(
        partial(scatter_kernel, len(parts), chunks),
        in_specs=[pl.BlockSpec(memory_space=pl.ANY)] * len(parts) + [vmem],
        out_specs=[vmem] * (len(parts) + 1),
        out_shape=[jax.ShapeDtypeStruct((rows, width), F32) for width in columns]
        + [jax.ShapeDtypeStruct((lines, 128), F32)],
        scratch_shapes=[
            *blocks(4), *blocks(4), *blocks(2), *blocks(), *blocks(), *blocks(),
            pltpu.VMEM((10, lines, 128), F32),
            dma((count, 4)), dma((count, 4)), dma((count, 4)), dma((count, 2)), dma((count, 2)),
            dma((count,)), dma((count,)), dma((count, LINE)), dma((count, LINE)), dma((count, LINE)),
            dma((count, LINE)), dma((5,)), dma((5,)),
        ],
        compiler_params=pltpu.CompilerParams(collective_id=1, has_side_effects=True),
        cost_estimate=pl.CostEstimate(flops=0, bytes_accessed=sent, transcendentals=0),
        name="scatter_blocks",
    )(*[part.reshape(mp, LINE, 2, 2, rows, part.shape[-1]) for part in parts], padded)
    return outs, summed.reshape(-1)[: vector.shape[0]]


def gradient_kernel(count, left_ref, *refs):
    rights, out_ref = refs[:count], refs[count]
    columns = rights[0].shape[0]
    for j in range(count):

        @pl.when(pl.program_id(0) == j)
        def _():
            out_ref[0, :, :columns] = dot(left_ref[...], rights[j][...], 1, 1).astype(BF16)

    if columns < out_ref.shape[2]:
        extra = out_ref.shape[2] - columns
        out_ref[0, :, columns:] = jnp.zeros((out_ref.shape[1], extra), BF16)


def weight_gradient(left, rights, lanes):
    width, tokens = left.shape
    count, columns = len(rights), rights[0].shape[0]
    padded = columns + -columns % lanes
    tile = 384
    whole = lambda j, m: (0, 0)
    return pl.pallas_call(
        partial(gradient_kernel, count),
        grid=(count, width // tile),
        in_specs=[pl.BlockSpec((tile, tokens), lambda j, m: (m, 0))]
        + [pl.BlockSpec((columns, tokens), whole)] * count,
        out_specs=pl.BlockSpec((1, tile, padded), lambda j, m: (j, m, 0)),
        out_shape=jax.ShapeDtypeStruct((count, width, padded), BF16),
        cost_estimate=pl.CostEstimate(
            flops=2 * width * tokens * columns * count,
            bytes_accessed=2 * count * (width * padded + columns * tokens) + 2 * width * tokens,
            transcendentals=0,
        ),
        name="weight_gradient",
    )(left, *rights)


def local_norm(values):
    centre = jnp.mean(values, axis=1, keepdims=True)
    centred = values - centre
    rstd = lax.rsqrt(jnp.mean(centred * centred, axis=1, keepdims=True) + EPSILON)
    return centred * rstd, rstd


def norm_backward(grad_normed, normed, rstd, gain):
    scaled = grad_normed * gain
    mean_grad = jnp.mean(scaled, axis=1, keepdims=True)
    mean_cross = jnp.mean(scaled * normed, axis=1, keepdims=True)
    return rstd * (scaled - mean_grad - normed * mean_cross)


def gelu_parts(rows):
    base = math.sqrt(2.0 / math.pi)
    square = rows * rows
    share = 0.5 * jnp.tanh(rows * (base + (base * 0.044715) * square)) + 0.5
    value = rows * share
    slope = share + value * (1.0 - share) * (2.0 * base + (6.0 * base * 0.044715) * square)
    return value, slope


def total(parts):
    out = parts[0]
    for part in parts[1:]:
        out = out + part
    return out


def body(
    inputs,
    picture_start,
    prenorm_gain,
    prenorm_shift,
    query_weight,
    query_bias,
    key_weight,
    value_weight,
    value_bias,
    output_weight,
    output_bias,
    midnorm_gain,
    midnorm_shift,
    hidden_weight,
    hidden_bias,
    project_weight,
    project_bias,
    cotangent,
    *,
    dp,
    mp,
):
    tokens, width = inputs.shape
    shard = query_weight.shape[1]
    hidden = hidden_weight.shape[1]
    group = HALF // tokens
    me = lax.axis_index("mp")
    groups = [list(range(i, i + group)) for i in range(0, mp, group)]

    fitted = dp == 16 and mp == 2
    lanes = 256

    def gather(weight):
        whole = lax.all_gather(weight, ("mp", "dp"), axis=0, tiled=True)
        return whole.reshape(mp, width, weight.shape[1])

    def scatter(parts, columns):
        whole = parts.reshape(mp * width, parts.shape[2])
        mine = lax.psum_scatter(whole, ("mp", "dp"), scatter_dimension=0, tiled=True)
        return lax.optimization_barrier(mine)[:, :columns].astype(F32)

    def to_heads(part):
        kinds = part.shape[0]
        if group == 1:
            return part
        part = part.reshape(kinds, group, HEADS // group, HEAD, tokens).transpose(1, 0, 2, 3, 4)
        part = lax.all_to_all(part, "mp", 0, 0, axis_index_groups=groups, tiled=True)
        return part.transpose(1, 2, 3, 0, 4).reshape(kinds, HEADS // group, HEAD, HALF)

    def from_heads(part):
        kinds = part.shape[0]
        if group == 1:
            return part
        part = part.reshape(kinds, HEADS // group, HEAD, group, tokens).transpose(3, 0, 1, 2, 4)
        part = lax.all_to_all(part, "mp", 0, 0, axis_index_groups=groups, tiled=True)
        return part.transpose(1, 0, 2, 3, 4).reshape(kinds, HEADS, HEAD, tokens)

    half = me // group
    starts = lax.dynamic_slice_in_dim(picture_start, half * HALF, HALF)
    masks = picture_masks(starts)

    attn_shard = jnp.concatenate([query_weight, key_weight, value_weight], axis=1)
    biases = jnp.concatenate([query_bias, value_bias, hidden_bias])
    if fitted:
        lines = jnp.pad(biases, (0, -biases.shape[0] % 1024)).reshape(-1, 128)
        (attn_weights, output_all), both = gather_blocks(
            [attn_shard, output_weight.T], (2, 2), lines, mp
        )
        biases_all = both.reshape(mp, -1)
        attn_weights, hidden_shard, project_shard = lax.optimization_barrier(
            (attn_weights, hidden_weight, project_weight)
        )
    else:
        attn_weights, output_all = gather(attn_shard), gather(output_weight.T)
        hidden_shard, project_shard = hidden_weight, project_weight
        biases_all = lax.all_gather(biases, "mp", axis=0, tiled=False)
    query_bias_all = biases_all[:, :shard]
    value_bias_all = biases_all[:, shard : 2 * shard]
    hidden_bias_all = biases_all[:, 2 * shard : 2 * shard + hidden]
    hidden_all = gather(hidden_shard)
    project_all = gather(project_shard.T)

    residual_in = inputs.astype(F32)
    normed_pre, rstd_pre = local_norm(residual_in)
    attn_in = (normed_pre * prenorm_gain + prenorm_shift).astype(BF16)

    stacks = []
    for j in range(mp):
        bias = jnp.concatenate(
            [query_bias_all[j], jnp.zeros((shard,), F32), value_bias_all[j]], axis=0
        )
        rows = (dot(attn_weights[j], attn_in, 0, 1) + bias[:, None]).astype(BF16)
        stacks.append(rows.reshape(3, shard // HEAD, HEAD, tokens))
    if group == 1:
        pieces = stacks
    else:
        pieces = [to_heads(jnp.concatenate(stacks, axis=1))]
    mixed_pieces, log_pieces, tops = [], [], []
    for piece in pieces:
        mixed_piece, log_piece, top_piece = attention_forward(masks, piece)
        mixed_pieces.append(mixed_piece)
        log_pieces.append(log_piece)
        tops.append(jnp.max(top_piece, axis=(1, 2)))
    peak_here = jnp.concatenate(tops) / LOG2E
    if group == 1:
        mixed = [piece.reshape(shard, tokens) for piece in mixed_pieces]
    else:
        rows = from_heads(mixed_pieces[0][None])[0].reshape(mp, shard, tokens)
        mixed = [rows[j] for j in range(mp)]
        spread = jnp.full((HEADS,), MASKED_SCORE, F32)
        peak_here = lax.dynamic_update_slice_in_dim(
            spread, peak_here, (me % group) * (HEADS // group), 0
        )
    residual_mid = (
        residual_in + total([dot(mixed[j], output_all[j], 0, 1) for j in range(mp)]) + output_bias
    )
    normed_mid, rstd_mid = local_norm(residual_mid)
    mlp_in = (normed_mid * midnorm_gain + midnorm_shift).astype(BF16)
    activated, slopes = [], []
    for j in range(mp):
        value, slope = gelu_parts(dot(hidden_all[j], mlp_in, 0, 1) + hidden_bias_all[j][:, None])
        activated.append(value.astype(BF16))
        slopes.append(slope.astype(BF16))
    activated, slopes = lax.optimization_barrier((activated, slopes))
    project_parts = weight_gradient(cotangent.T, activated, lanes)
    project_parts, late_cotangent = lax.optimization_barrier((project_parts, cotangent))
    with jax.named_scope("scatter_project"):
        project_grad = scatter(project_parts, hidden)
    grad_up = [
        (dot(project_all[j], late_cotangent, 0, 1) * slopes[j].astype(F32)).astype(BF16)
        for j in range(mp)
    ]
    grad_up = lax.optimization_barrier(grad_up)
    hidden_parts = weight_gradient(mlp_in.T, grad_up, lanes)
    hidden_parts, grad_up, activated = lax.optimization_barrier((hidden_parts, grad_up, activated))
    with jax.named_scope("scatter_hidden"):
        hidden_grad = scatter(hidden_parts, hidden)
    final_rows = (
        residual_mid
        + total([dot(activated[j], project_all[j], 0, 1) for j in range(mp)])
        + project_bias
    )
    layer_output = final_rows.astype(BF16)

    grad_output = cotangent.astype(F32)
    grad_mid = total([dot(grad_up[j], hidden_all[j], 0, 1) for j in range(mp)])
    grad_resid = grad_output + norm_backward(grad_mid, normed_mid, rstd_mid, midnorm_gain)
    grad_branch = grad_resid.astype(BF16)
    output_parts = weight_gradient(grad_branch.T, mixed, 1 if fitted else lanes)
    grad_mixed = [
        dot(output_all[j], grad_branch, 0, 1).astype(BF16).reshape(shard // HEAD, HEAD, tokens)
        for j in range(mp)
    ]
    if group > 1:
        grad_mixed = [to_heads(jnp.concatenate(grad_mixed, axis=0)[None])[0]]
    grad_pieces = [
        attention_backward(masks, piece, mixed_piece, log_piece, grads)
        for piece, mixed_piece, log_piece, grads in zip(
            pieces, mixed_pieces, log_pieces, grad_mixed
        )
    ]
    if group > 1:
        whole = from_heads(grad_pieces[0]).reshape(3, mp, shard // HEAD, HEAD, tokens)
        grad_pieces = [whole[:, j] for j in range(mp)]
    grad_rows = [piece.reshape(3 * shard, tokens) for piece in grad_pieces]
    attn_parts = weight_gradient(attn_in.T, grad_rows, 1 if fitted else lanes)
    grad_pre = total([dot(grad_rows[j], attn_weights[j], 0, 1) for j in range(mp)])
    inputs_gradient = grad_resid + norm_backward(grad_pre, normed_pre, rstd_pre, prenorm_gain)

    row_sums = [jnp.sum(rows.astype(F32), axis=1) for rows in grad_rows]
    head_parts = (
        jnp.stack([sums[:shard] for sums in row_sums]),
        jnp.stack([sums[2 * shard :] for sums in row_sums]),
        jnp.stack([jnp.sum(part.astype(F32), axis=1) for part in grad_up]),
    )
    norm_parts = (
        jnp.sum(grad_pre * normed_pre, axis=0),
        jnp.sum(grad_pre, axis=0),
        jnp.sum(grad_branch.astype(F32), axis=0),
        jnp.sum(grad_mid * normed_mid, axis=0),
        jnp.sum(grad_mid, axis=0),
        jnp.sum(grad_output, axis=0),
    )
    slot = lax.axis_index("dp") * mp + me
    peak_slots = jnp.where(lax.iota(jnp.int32, dp * mp)[:, None] == slot, peak_here[None, :], 0.0)
    flat = jnp.concatenate([item.reshape(-1) for item in (*head_parts, *norm_parts, peak_slots)])
    if fitted:
        output_parts, project_grad = lax.optimization_barrier((output_parts, project_grad))
        (attn_grad, output_grad), flat = scatter_blocks([attn_parts, output_parts], (2, 2), flat, mp)
    else:
        attn_grad, output_grad = scatter(attn_parts, 3 * shard), scatter(output_parts, shard)
        flat = lax.psum(flat, ("dp", "mp"))
    ends = [mp * shard, mp * shard, mp * hidden] + [width] * 6
    sums, at = [], 0
    for size in ends:
        sums.append(flat[at : at + size])
        at += size
    peak_all = jnp.max(flat[at:].reshape(dp * mp, HEADS), axis=0)
    logit_peak = lax.dynamic_slice_in_dim(peak_all, me * (HEADS // mp), HEADS // mp)
    factor = jnp.repeat(jnp.sqrt(CLIP_LIMIT / jnp.maximum(logit_peak, CLIP_LIMIT)), HEAD)
    clipped_query = query_weight.astype(F32) * factor[None, :]
    clipped_key = key_weight.astype(F32) * factor[None, :]
    query_bias_grad, value_bias_grad, hidden_bias_grad = (
        lax.dynamic_index_in_dim(item.reshape(mp, -1), me, keepdims=False) for item in sums[:3]
    )
    return (
        layer_output,
        inputs_gradient,
        sums[3],
        sums[4],
        attn_grad[:, :shard],
        query_bias_grad,
        attn_grad[:, shard : 2 * shard],
        attn_grad[:, 2 * shard :],
        value_bias_grad,
        output_grad.T,
        sums[5],
        sums[6],
        sums[7],
        hidden_grad,
        hidden_bias_grad,
        project_grad.T,
        sums[8],
        logit_peak,
        clipped_query,
        clipped_key,
    )


def solution(mesh):
    rows = P(("dp", "mp"), None)
    split = P("dp", "mp")
    turned = P("mp", "dp")
    heads = P("mp")
    whole = P()
    placed = (
        rows, P("dp"), whole, whole, split, heads, split, split, heads, turned, whole, whole, whole,
        split, heads, turned, whole, rows,
    )
    given = (
        rows, rows, whole, whole, split, heads, split, split, heads, turned, whole, whole, whole,
        split, heads, turned, whole, heads, split, split,
    )
    return jax.shard_map(
        partial(body, dp=mesh.shape["dp"], mp=mesh.shape["mp"]),
        mesh=mesh,
        in_specs=placed,
        out_specs=given,
        check_vma=False,
    )
```
